32 devices in a mesh: row: 8 (over y, x, core), col: 4 (over z).
Axes of the slice: x: 2, y: 2, z: 4, core: 2. Of those that a mesh axis runs over, the one named last changes fastest.
Arguments:
- state: float32 [2048, 4, 1024], P('row', 'col'), may hold values from -6 to 6
- coupling: bfloat16 [2048, 4, 1024], P('row', 'col'), may hold values from -2 to 2, as said below
- coupling_t: bfloat16 [2, 2048, 4, 1024], P(None, 'row', 'col'), may hold values from -2 to 2, as said below
- factor: float32 [4, 4, 256, 256], P(None, 'col', 'row'), may hold values from -0.3 to 1.3
- cofactor: float32 [4, 4, 256, 256], P(None, 'col', 'row'), may hold values from -0.3 to 1.3
- rates: float32 [4, 4, 256], P(None, 'col'), may hold values from 0.5 to 2
Outputs:
- updated_state: float32 [2048, 4, 1024], P('row', 'col')
The draws below stay inside these ranges and needn't reach their ends.
Inputs may be any that keep to these rules, and one draw needn't show every extreme that they name: coupling and coupling_t hold the same matrix A; its blocks A(i, k) are zero unless k > i. coupling_t holds the transposed blocks of the A in coupling.
All inputs are finite; a program needn't handle non-finite values.
Results may differ from the reference program's by a relative error of at most 0.0003.
Values may be sent and summed in bfloat16 or wider, within the bound.
A program may use at most 64 MiB of HBM per device.

```python
import math
import jax
import jax.numpy as jnp
from jax import lax

BS = 256
STEPS = 2
NBH = 8
NB = 16
CB = 4
N_COL = 4


def coupling_blocks(seed_key, block_rows, block_cols):
    base_key = jax.random.fold_in(seed_key, 404)
    flat_rows = block_rows.reshape(-1).astype(jnp.int32)
    flat_cols = block_cols.reshape(-1).astype(jnp.int32)
    limit = 4.0 / math.sqrt(BS)

    def one_block(row_id, col_id):
        sub_key = jax.random.fold_in(base_key, row_id * NB + col_id)
        values = jax.random.normal(sub_key, (BS, BS), jnp.float32) / math.sqrt(BS)
        values = jnp.clip(values, -limit, limit)
        return jnp.where(col_id > row_id, values, 0.0)
    drawn = jax.vmap(one_block)(flat_rows, flat_cols)
    return drawn.reshape(block_rows.shape + (BS, BS))


def draw_coupling(key, part):
    col_count = NB // CB
    row_ids = jnp.arange(NBH, dtype=jnp.int32)[:, None, None]
    stored = (jnp.arange(CB, dtype=jnp.int32)[:, None] * col_count + jnp.arange(col_count, dtype=jnp.int32)[None, :])[None]
    block_rows = jnp.broadcast_to(row_ids, (NBH, CB, col_count))
    block_cols = jnp.broadcast_to(NB - 1 - stored, (NBH, CB, col_count))
    drawn = coupling_blocks(key, block_rows, block_cols)
    drawn = jnp.transpose(drawn, (0, 3, 2, 1, 4))
    return drawn.reshape(NBH * BS, col_count, CB * BS).astype(jnp.bfloat16)


def draw_coupling_t(key, part):
    col_count = NB // CB
    rotated = (jnp.arange(NBH, dtype=jnp.int32) + NBH // 2) % NBH
    stored_rows = jnp.arange(2, dtype=jnp.int32)[:, None] * NBH + rotated[None, :]
    stored_cols = jnp.arange(CB, dtype=jnp.int32)[:, None] * col_count + jnp.arange(col_count, dtype=jnp.int32)[None, :]
    block_rows = jnp.broadcast_to(stored_cols[None, None], (2, NBH, CB, col_count))
    block_cols = jnp.broadcast_to((NB - 1 - stored_rows)[:, :, None, None], (2, NBH, CB, col_count))
    drawn = coupling_blocks(key, block_rows, block_cols)
    drawn = jnp.swapaxes(drawn, -1, -2)
    drawn = jnp.transpose(drawn, (0, 1, 4, 3, 2, 5))
    return drawn.reshape(2, NBH * BS, col_count, CB * BS).astype(jnp.bfloat16)


def operator_draw(seed_key):
    col_count = NB // CB
    perturb = jax.random.normal(seed_key, (CB, col_count, BS, BS), jnp.float32)
    perturb = jnp.clip(0.3 * perturb / math.sqrt(BS), -0.3, 0.3)
    return jnp.eye(BS, dtype=jnp.float32) + perturb


def draw_factor(key, part):
    return operator_draw(jax.random.fold_in(key, 17))


def draw_cofactor(key, part):
    return operator_draw(jax.random.fold_in(key, 29))


def block_scale(own_key, dims, shards, least, largest):
    gain = 1.0
    for axis_at, blocks in shards:
        steps = jax.random.uniform(jax.random.fold_in(jax.random.fold_in(own_key, 6), axis_at), (blocks,), jnp.float32, least / len(shards), largest / len(shards))
        gain = gain * jnp.repeat(jnp.exp(steps), dims[axis_at] // blocks).reshape((-1,) + (1,) * (len(dims) - 1 - axis_at))
    return gain


def centred(stream_key, dims, scale, bound, pieces=(), held_as=jnp.bfloat16):
    entries = jax.random.normal(stream_key, dims, jnp.float32) * scale
    if len(pieces) > 0:
        entries = block_scale(stream_key, dims, pieces, -0.22, 0.18) * entries
    return jnp.clip(entries, min=-bound, max=bound).astype(held_as)


def setup_inputs(seed: int = 0) -> dict:
    key_list = jax.random.split(jax.random.key(seed), 7)
    state = centred(key_list[0], (NBH * BS, N_COL, CB * BS), 1.0, 6.0, ((0, 8), (1, 4)), jnp.float32)
    coupling = draw_coupling(jax.random.fold_in(key_list[6], 71), 0)
    coupling_t = draw_coupling_t(jax.random.fold_in(key_list[6], 71), 0)
    factor = draw_factor(jax.random.fold_in(key_list[6], 71), 0)
    cofactor = draw_cofactor(jax.random.fold_in(key_list[6], 71), 0)
    rates = jnp.clip(jnp.exp(math.log(2.0) - 1.3862944 * jax.random.uniform(key_list[5], (CB, N_COL, BS), jnp.float32) ** block_scale(key_list[5], (CB, N_COL, BS), ((1, 4),), -0.2, 0.2)), 0.5, 2.0)
    return {"state": state, "coupling": coupling, "coupling_t": coupling_t, "factor": factor, "cofactor": cofactor, "rates": rates}


HIGHEST_PRECISION = lax.Precision.HIGHEST


def to_blocks(flattened, row_total):
    col_count = flattened.shape[1]
    shaped = flattened.reshape(row_total, BS, col_count, CB, BS)
    shaped = jnp.transpose(shaped, (0, 3, 2, 1, 4))
    return shaped.reshape(row_total, CB * col_count, BS, BS)


def from_blocks(blocks):
    row_total = blocks.shape[0]
    col_count = blocks.shape[1] // CB
    shaped = blocks.reshape(row_total, CB, col_count, BS, BS)
    shaped = jnp.transpose(shaped, (0, 3, 2, 1, 4))
    return shaped.reshape(row_total * BS, col_count, CB * BS)


def solve_block(residual, left_p, left_q, left_e, right_p, right_q, right_e):
    middle = jnp.dot(left_q, residual, precision=HIGHEST_PRECISION, preferred_element_type=jnp.float32)
    middle = jnp.dot(middle, right_q.T, precision=HIGHEST_PRECISION, preferred_element_type=jnp.float32)
    middle = middle / (left_e[:, None] + right_e[None, :])
    product = jnp.dot(left_p, middle, precision=HIGHEST_PRECISION, preferred_element_type=jnp.float32)
    return -jnp.dot(product, right_p.T, precision=HIGHEST_PRECISION, preferred_element_type=jnp.float32)


def reference(state, coupling, coupling_t, factor, cofactor, rates):
    col_count = state.shape[1]
    half_rows = NBH // 2
    blocks = to_blocks(state, NBH)
    upper_blocks = to_blocks(coupling, NBH)
    lower_blocks = to_blocks(coupling_t.reshape(NB * BS, col_count, CB * BS), NB)
    all_p = factor.reshape(NB, BS, BS)
    all_q = cofactor.reshape(NB, BS, BS)
    all_e = rates.reshape(NB, BS)
    row_ids = jnp.arange(NBH, dtype=jnp.int32)
    col_ids = jnp.arange(NB, dtype=jnp.int32)
    for wave_step in range(STEPS):
        antidiag = NB - 1 - wave_step
        partner = (antidiag - row_ids).astype(jnp.int32)
        usable = row_ids <= partner
        residual = blocks[row_ids, partner]
        solution = jax.vmap(solve_block)(residual, all_p[:NBH], all_q[:NBH], all_e[:NBH], all_p[partner], all_q[partner], all_e[partner])
        solution = jnp.where(usable[:, None, None], solution, 0.0)
        blocks = blocks.at[row_ids, partner].set(jnp.where(usable[:, None, None], solution, residual))
        mirror = (antidiag - col_ids).astype(jnp.int32)
        use_row = mirror <= col_ids
        sources = jnp.clip(jnp.where(use_row, mirror, col_ids), 0, NBH - 1).astype(jnp.int32)
        chosen = solution[sources]
        partner_blocks = jnp.where(use_row[:, None, None], chosen, jnp.swapaxes(chosen, 1, 2))
        upper_pick = jnp.clip(wave_step + col_ids, 0, NB - 1).astype(jnp.int32)

        def update_row(row_args, wave_step=wave_step, antidiag=antidiag, partner_blocks=partner_blocks, upper_pick=upper_pick):
            row_id, row_blocks, row_solution = row_args
            needed = wave_step + row_id
            stored = ((needed % NBH + half_rows) % NBH + NBH * (needed // NBH)).astype(jnp.int32)
            coupled = upper_blocks[row_id][upper_pick].astype(jnp.float32)
            transposed = lower_blocks[stored].astype(jnp.float32)
            left_terms = jnp.einsum("mab,mbc->mac", coupled, partner_blocks, precision=HIGHEST_PRECISION)
            right_terms = jnp.einsum("ab,mbc->mac", row_solution, transposed, precision=HIGHEST_PRECISION)
            targets = (row_id <= col_ids) & (row_id + col_ids < antidiag)
            return row_blocks - jnp.where(targets[:, None, None], left_terms + right_terms, 0.0)

        blocks = lax.map(update_row, (row_ids, blocks, solution))
    return from_blocks(blocks)
```

```python
import functools

import jax
import jax.numpy as jnp
from jax import lax
from jax.experimental import pallas as pl
from jax.experimental.pallas import tpu as pltpu
from jax.sharding import PartitionSpec as P

STEPS = 2
CHUNKS = 4
MESH = pl.DeviceIdType.MESH
F32 = jnp.float32
NN = (((1,), (0,)), ((), ()))
NT = (((1,), (1,)), ((), ()))


def halves(x):
    hi = x.astype(jnp.bfloat16)
    return hi, (x - hi.astype(F32)).astype(jnp.bfloat16)


def mm(a, b, dims):
    return lax.dot_general(a, b, dims, preferred_element_type=F32)


def dot3(a, b, dims):
    ah, al = halves(a)
    bh, bl = halves(b)
    return mm(ah, bh, dims) + (mm(ah, bl, dims) + mm(al, bh, dims))


def kernel(R, C, U, BS, SR, state, upper, lower, factor, cofactor, rates, out,
           ops, ebuf, xz, atb, an, ops_sem, e_sem, xz_sem, at_sem, an_sem, send_sem):
    H = R // 2
    r = lax.axis_index("row")
    c = lax.axis_index("col")
    d = [2 * R - 1 - s for s in range(STEPS)]

    def owner(row, s):
        return (d[s] - row) % C

    o = [owner(r, s) for s in range(STEPS)]
    sends = []
    me = r * C + c

    barrier = pltpu.get_barrier_semaphore()

    @pl.loop(1, R * C)
    def _(k):
        peer = (me + k) % (R * C)
        pl.semaphore_signal(barrier, inc=1, device_id=(peer // C, peer % C), device_id_type=MESH)

    pl.semaphore_wait(barrier, R * C - 1)

    def send(cond, src, dst, sem, dev):
        copy = pltpu.make_async_remote_copy(
            src_ref=src, dst_ref=dst, send_sem=send_sem.at[0], recv_sem=sem,
            device_id=dev, device_id_type=MESH)
        sends.append((cond, copy))

        @pl.when(cond)
        def _():
            copy.start()

    def send_or_local(cond, src, dst, sem, dev):
        mine = (dev[0] == r) & (dev[1] == c)
        send(cond & jnp.logical_not(mine), src, dst, sem, dev)

        @pl.when(cond & mine)
        def _():
            pltpu.make_async_copy(src, dst, sem).start()

    def arrive(ref, sem):
        pltpu.make_async_copy(ref, ref, sem).wait()

    def slot(u):
        if isinstance(u, int):
            return pl.ds(u * BS, BS)
        return pl.ds(pl.multiple_of(u * BS, BS), BS)

    def target(row, m, s):
        return (row <= m) & (row + m < d[s])

    rows = pl.ds(pl.multiple_of(r * SR, SR), SR)

    def send_operators(s):
        for src, base in ((cofactor, 0), (factor, 2)):
            for u in range(U):
                m = c + C * u
                if u >= U // 2 - s:
                    to = d[s] - m
                    send_or_local((to >= 0) & (to < R), src.at[u], ops.at[base + 1, rows],
                                  ops_sem.at[base + 1], (to, c))
                if u < U // 2:
                    send_or_local(m < R, src.at[u], ops.at[base, rows],
                                  ops_sem.at[base], (m, owner(m, s)))

    def from_upper(u):
        return (u + 1) * C <= H

    def send_lower(s, slots):
        to = (r + R - s - H) % R
        for u in slots:
            if not from_upper(u):
                m = c + C * u
                send(target(to, m, s) & (to + s < R), lower.at[0, :, slot(u)], atb.at[s, u],
                     at_sem.at[s, u], (to, c))

    def send_plain(s):
        m = r
        to_u = jnp.minimum(m // C, U - 1)
        for u in range(H // C + 1):
            i = c + C * u - s
            reach = (i >= 0) & (m < (H // C) * C) & target(i, m, s)
            send_or_local(reach, upper.at[:, slot(u)], atb.at[s, to_u],
                          at_sem.at[s, to_u], (i, m % C))

    def send_upper():
        for u in range(U):
            m = c + C * u - 1
            to = (c + C - 1) % C
            to_u = jnp.maximum(jnp.where(c >= 1, u, u - 1), 0)
            send((m >= 0) & target(r, m, 1), upper.at[:, slot(u)], an.at[to_u],
                 an_sem.at[to_u], (r, to))

    for s in range(STEPS):
        send_or_local(c == r % C, rates, ebuf, e_sem.at[0], (r, o[s]))
    send_operators(0)
    send_lower(0, range(U - 1, U // 2 - 1, -1))
    send_operators(1)
    send_plain(0)
    out[...] = state[...]

    def spread(s, h, who):
        own_col = r % C == c
        k = jnp.where(own_col, r // C, (d[s] - r) // C)
        has = (own_col | (c == o[s])) & who

        def give(cond, to):
            send(cond & has, xz.at[s, U, part(h)], xz.at[s, k, part(h)], xz_sem.at[s, k, h], (to, c))

        give(r % 2 == 1, jnp.maximum(r - 1, 0))
        for back in range(1, R // 2):
            pair = r // 2 - back
            give(pair >= 0, jnp.maximum(2 * pair + 1 - r % 2, 0))

    def part(h):
        return pl.ds(h * (BS // CHUNKS), BS // CHUNKS)

    def pass_row(s, h, who=True):
        block = xz.at[s, U, part(h)]
        sem = xz_sem.at[s, U, h]
        far = o[s] == 0
        up = (c >= o[s]) & (c < C - 1)
        if s == 0:
            send((c == o[s]) & far & who, block, block, sem, (r, C - 1))
            up = up & jnp.logical_not(far & (c == C - 2))
        send((c <= o[s]) & (c >= 1) & who, block, block, sem, (r, jnp.maximum(c - 1, 0)))
        send(up & who, block, block, sem, (r, jnp.minimum(c + 1, C - 1)))

    def take_row(s):
        other = c != o[s]
        for h in range(CHUNKS):
            @pl.when(other)
            def _(h=h):
                arrive(xz.at[s, U, part(h)], xz_sem.at[s, U, h])

            pass_row(s, h, other)
            spread(s, h, other)

    def give_row(s):
        for h in range(CHUNKS):
            pass_row(s, h, c == o[s])
            spread(s, h, c == o[s])

    def solve(s):
        q = (d[s] - r) // C
        arrive(ebuf, e_sem.at[0])
        left_e = jnp.transpose(jnp.broadcast_to(ebuf[pl.ds(r // C, 1), :], (BS, BS)))
        rate = left_e + rates[pl.ds(q, 1), :]
        arrive(ops.at[0], ops_sem.at[0])
        mid = dot3(ops[0], out[:, slot(q)], NN)
        arrive(ops.at[1], ops_sem.at[1])
        mid = dot3(mid, ops[1], NT) / rate
        arrive(ops.at[2], ops_sem.at[2])
        mid = dot3(ops[2], mid, NN)
        arrive(ops.at[3], ops_sem.at[3])
        x = -dot3(mid, ops[3], NT)
        xz[s, U] = x
        out[:, slot(q)] = x

    def z_index(u, s):
        m = c + C * u
        j = jnp.where(d[s] - m <= m, d[s] - m, m)
        k = jnp.where(j == r, U, jnp.where(j % C == c, j // C, u))
        return j, k

    def collect(u, s, extra=True):
        j, k = z_index(u, s)
        landed = r < j
        if u >= U // 2:
            landed = landed & (j % C != c)
        landed = landed & extra

        for h in range(CHUNKS):
            block = xz.at[s, u, part(h)]

            @pl.when(landed)
            def _(block=block, h=h):
                arrive(block, xz_sem.at[s, u, h])

            send(landed & (r // 2 < j // 2) & (r % 2 != j % 2), block, block,
                 xz_sem.at[s, u, h], (r + 1 - 2 * (r % 2), c))

    def right(u, s):
        arrive(atb.at[s, u], at_sem.at[s, u])
        xh, xl = halves(xz[s, U])
        at = atb[s, u]
        dims = NT if from_upper(u) else NN
        out[:, slot(u)] -= mm(xh, at, dims) + mm(xl, at, dims)

    def left(u, s):
        m = c + C * u
        j, k = z_index(u, s)
        if s > 0:
            arrive(an.at[u], an_sem.at[u])
            a = an[u]
        else:
            a = upper[:, slot(u)]
        zh, zl = halves(xz[s, k])

        def apply(dims):
            out[:, slot(u)] -= mm(a, zh, dims) + mm(a, zl, dims)

        low, high = C * u, C * u + C - 1
        if 2 * low >= d[s]:
            apply(NN)
        elif 2 * high < d[s]:
            apply(NT)
        else:
            straight = d[s] - m <= m
            pl.when(straight)(lambda: apply(NN))
            pl.when(jnp.logical_not(straight))(lambda: apply(NT))

    def on_targets(s, fns, but=None):
        for u in range(U):
            live = target(r, c + C * u, s)
            if but is not None:
                live = live & jnp.logical_not(but(u))

            @pl.when(live)
            def _(u=u):
                for fn in fns:
                    fn(u, s)

    @pl.when(c == o[0])
    def _():
        solve(0)

    give_row(0)
    take_row(0)
    send_upper()
    send_lower(0, range(U // 2 - 1, -1, -1))
    send_lower(1, range(U - 1, -1, -1))
    send_plain(1)

    q1 = (d[1] - r) // C
    first = c == o[1]

    def picked(u):
        return first & (q1 == u)

    for u in range(U // 2 - 1, U):
        collect(u, 0, picked(u))

        @pl.when(picked(u))
        def _(u=u):
            right(u, 0)
            left(u, 0)

    @pl.when(first)
    def _():
        solve(1)

    give_row(1)

    def rest():
        on_targets(0, (right, left), picked)

    for u in range(U):
        collect(u, 0, jnp.logical_not(picked(u)))
    rest()

    take_row(1)
    on_targets(1, (right,))
    for u in range(U):
        collect(u, 1)
    on_targets(1, (left,))

    for cond, copy in sends:
        @pl.when(cond)
        def _(copy=copy):
            copy.wait_send()


def on_device(state, coupling, coupling_t, factor, cofactor, rates):
    R = lax.axis_size("row")
    C = lax.axis_size("col")
    U = 2 * R // C
    BS = state.shape[0]
    SR = factor.shape[2]
    flat = U * BS
    vmem = pl.BlockSpec(memory_space=pltpu.VMEM)
    hbm = pl.BlockSpec(memory_space=pl.ANY)
    dma = pltpu.SemaphoreType.DMA
    out = pl.pallas_call(
        functools.partial(kernel, R, C, U, BS, SR),
        out_shape=jax.ShapeDtypeStruct((BS, flat), F32),
        in_specs=[vmem, vmem, hbm, vmem, vmem, vmem],
        out_specs=vmem,
        scratch_shapes=[
            pltpu.VMEM((4, BS, BS), F32),
            pltpu.VMEM((U, BS), F32),
            pltpu.VMEM((STEPS, U + 1, BS, BS), F32),
            pltpu.VMEM((STEPS, U, BS, BS), jnp.bfloat16),
            pltpu.VMEM((U, BS, BS), jnp.bfloat16),
            dma((4,)),
            dma((1,)),
            dma((STEPS, U + 1, CHUNKS)),
            dma((STEPS, U)),
            dma((U,)),
            dma((1,)),
        ],
        compiler_params=pltpu.CompilerParams(
            collective_id=0, has_side_effects=True, vmem_limit_bytes=48 * 1024 * 1024),
    )(
        state.reshape(BS, flat),
        coupling.reshape(BS, flat),
        coupling_t.reshape(coupling_t.shape[0], BS, flat),
        factor.reshape(U, SR, BS),
        cofactor.reshape(U, SR, BS),
        rates.reshape(U, BS),
    )
    return out.reshape(BS, 1, flat)


def solution(mesh):
    return jax.shard_map(
        on_device,
        mesh=mesh,
        in_specs=(
            P("row", "col", None),
            P("row", "col", None),
            P(None, "row", "col", None),
            P(None, "col", "row", None),
            P(None, "col", "row", None),
            P(None, "col", None),
        ),
        out_specs=P("row", "col", None),
        check_vma=False,
    )
```

```python
import functools

import jax
import jax.numpy as jnp
from jax import lax
from jax.experimental import pallas as pl
from jax.experimental.pallas import tpu as pltpu
from jax.sharding import PartitionSpec as P

STEPS = 2
PARTS = 2
PAD = 16
OP_MAX = 1.3
MESH = pl.DeviceIdType.MESH
F32 = jnp.float32
BF16 = jnp.bfloat16
NN = (((1,), (0,)), ((), ()))
NT = (((1,), (1,)), ((), ()))
scope = jax.named_scope


def halves(x):
    hi = x.astype(BF16)
    return hi, (x - hi.astype(F32)).astype(BF16)


def mm(a, b, dims):
    return lax.dot_general(a, b, dims, preferred_element_type=F32)


def dot3(a, b, dims):
    ah, al = halves(a)
    bh, bl = halves(b)
    return mm(ah, bh, dims) + (mm(ah, bl, dims) + mm(al, bh, dims))


def encode(x, inverse):
    v = jnp.exp2(jnp.sqrt(jnp.abs(x) * inverse) * 250.0 - 125.0)
    return jnp.where(x < 0, -v, v).astype(BF16)


def decode(v, scale):
    v = v.astype(F32)
    y = jnp.log2(jnp.abs(v)) * (1.0 / 250.0) + 0.5
    x = y * y * scale
    return jnp.where(v < 0, -x, x)


def kernel(R, C, U, BS, SR, state, upper_in, lower_in, factor, cofactor, rates_in, out,
           upper, lower, raw, rates, enc, ops, mats, ebuf, xz, own, atb, an,
           load_sem, ops_sem, e_sem, xz_sem, at_sem, an_sem, send_sem):
    H = R // 2
    r = lax.axis_index("row")
    c = lax.axis_index("col")
    d = [2 * R - 1 - s for s in range(STEPS)]

    def owner(row, s):
        return (d[s] - row) % C

    o = [owner(r, s) for s in range(STEPS)]
    sends = []
    me = r * C + c

    barrier = pltpu.get_barrier_semaphore()

    @pl.loop(1, R * C)
    def _(k):
        peer = (me + k) % (R * C)
        pl.semaphore_signal(barrier, inc=1, device_id=(peer // C, peer % C), device_id_type=MESH)

    pltpu.make_async_copy(cofactor, raw.at[0], load_sem.at[0]).start()
    pltpu.make_async_copy(factor, raw.at[1], load_sem.at[0]).start()
    pltpu.make_async_copy(rates_in.at[:, 0, :], rates, load_sem.at[1]).start()
    pltpu.make_async_copy(lower_in.at[0], lower, load_sem.at[2]).start()
    lanes = out.shape[1] // state.shape[1]
    for j in range(state.shape[1]):
        pltpu.make_async_copy(state.at[:, j, 0, :], out.at[:, pl.ds(j * lanes, lanes)], load_sem.at[3]).start()
    pltpu.make_async_copy(upper_in, upper, load_sem.at[4]).start()

    def arrive(ref, sem):
        pltpu.make_async_copy(ref, ref, sem).wait()

    def send(cond, src, dst, sem, dev):
        copy = pltpu.make_async_remote_copy(
            src_ref=src, dst_ref=dst, send_sem=send_sem.at[0], recv_sem=sem,
            device_id=dev, device_id_type=MESH)
        sends.append((cond, copy))

        @pl.when(cond)
        def _():
            copy.start()

    def send_or_local(cond, src, dst, sem, dev):
        mine = (dev[0] == r) & (dev[1] == c)
        send(cond & jnp.logical_not(mine), src, dst, sem, dev)

        @pl.when(cond & mine)
        def _():
            pltpu.make_async_copy(src, dst, sem).start()

    def slot(u):
        if isinstance(u, int):
            return pl.ds(u * BS, BS)
        return pl.ds(pl.multiple_of(u * BS, BS), BS)

    def target(row, m, s):
        return (row <= m) & (row + m < d[s])

    with scope("encode"):
        arrive(raw, load_sem.at[0])
        for u in range(U):
            both = jnp.concatenate([raw[0, u], raw[1, u]], axis=0)
            enc[u] = encode(both, 1.0 / OP_MAX)
        arrive(rates, load_sem.at[1])

    with scope("barrier"):
        pl.semaphore_wait(barrier, R * C - 1)

    def send_operators(s):
        for u in range(U):
            m = c + C * u
            if u >= U // 2 - s:
                to = d[s] - m
                send_or_local((to >= 0) & (to < R), enc.at[u], ops.at[1, r], ops_sem.at[1], (to, c))
            if u < U // 2:
                send_or_local(m < R, enc.at[u], ops.at[0, r], ops_sem.at[0], (m, owner(m, s)))

    def send_lower():
        to = (r + H) % R
        for u in range(U - 1, -1, -1):
            m = c + C * u
            send(target(to, m, 0) & (m != to), lower.at[:, slot(u)], atb.at[0, u], at_sem.at[0, u], (to, c))

    def send_upper(cond):
        for u in range(U):
            m = c + C * u - 1
            to = (c + C - 1) % C
            to_u = jnp.maximum(jnp.where(c >= 1, u, u - 1), 0)
            send(cond & (m >= 0) & target(r, m, 1), upper.at[:, slot(u)], an.at[to_u],
                 an_sem.at[to_u], (r, to))

    def hand_down(u):
        m = c + C * u
        live = (r >= 1) & (m >= r) & target(r - 1, m, 1)
        to = (jnp.maximum(r - 1, 0), c)
        if u < U // 2:
            send(live & (m == r), upper.at[:, slot(u)], atb.at[1, u], at_sem.at[1, u], to)
        send(live & (m != r), atb.at[0, u], atb.at[1, u], at_sem.at[1, u], to)

    with scope("sends0"):
        send_operators(0)
        for s in range(STEPS):
            send_or_local(c == r % C, rates, ebuf, e_sem.at[0], (r, o[s]))
        arrive(lower, load_sem.at[2])
        send_lower()
        send_operators(1)
        arrive(upper, load_sem.at[4])
        arrive(out, load_sem.at[3])
        send_upper((c != o[0]) & (c != o[1]))

    half = BS // PARTS

    def part(h):
        if h == 0:
            return pl.ds(0, PAD + half)
        return pl.ds(PAD + h * half, half)

    def spread(s, h, who):
        own_col = r % C == c
        k = jnp.where(own_col, r // C, (d[s] - r) // C)
        has = (own_col | (c == o[s])) & who

        def give(cond, to):
            send(cond & has, xz.at[s, U, part(h)], xz.at[s, k, part(h)], xz_sem.at[s, k, h], (to, c))

        give(r % 2 == 1, jnp.maximum(r - 1, 0))
        for back in range(1, R // 2):
            pair = r // 2 - back
            give(pair >= 0, jnp.maximum(2 * pair + 1 - r % 2, 0))

    def give_row(s):
        at = c == o[s]
        far = (o[s] == 0) & at
        for h in range(PARTS):
            block = xz.at[s, U, part(h)]
            sem = xz_sem.at[s, U, h]
            if s == 0:
                send(far, block, block, sem, (r, C - 1))
                send(at & (o[s] >= 1), block, block, sem, (r, jnp.maximum(c - 1, 0)))
                spread(s, h, at)
                send(at & (o[s] >= 2), block, block, sem, (r, jnp.maximum(c - 2, 0)))
                send(at & (o[s] <= C - 3) & jnp.logical_not(far & (C == 3)), block, block, sem, (r, jnp.minimum(c + 2, C - 1)))
                send(at & (o[s] <= C - 2), block, block, sem, (r, jnp.minimum(c + 1, C - 1)))
            else:
                send(at & (o[s] >= 2), block, block, sem, (r, jnp.maximum(c - 2, 0)))
                send(at & (o[s] <= C - 3), block, block, sem, (r, jnp.minimum(c + 2, C - 1)))
                spread(s, h, at)
                send(at & (o[s] >= 1), block, block, sem, (r, jnp.maximum(c - 1, 0)))
                send(at & (o[s] <= C - 2), block, block, sem, (r, jnp.minimum(c + 1, C - 1)))

    def take_row(s):
        other = c != o[s]
        down = (c <= o[s] - 2) & (c >= 1)
        up = (c >= o[s] + 2) & (c < C - 1)
        if s == 0:
            up = up & jnp.logical_not((o[s] == 0) & (c == C - 2))
        for h in range(PARTS):
            block = xz.at[s, U, part(h)]
            sem = xz_sem.at[s, U, h]

            @pl.when(other)
            def _(block=block, sem=sem):
                arrive(block, sem)

            send(down, block, block, sem, (r, jnp.maximum(c - 1, 0)))
            send(up, block, block, sem, (r, jnp.minimum(c + 1, C - 1)))
            spread(s, h, other)

    def decoded(s, k):
        return decode(xz[s, k, PAD:], xz[s, k, 0:1, :].astype(F32))

    def split_own(s):
        xh, xl = halves(decoded(s, U))
        own[0] = xh
        own[1] = xl

    def solve(s):
        q = (d[s] - r) // C
        with scope("w_e"):
            arrive(ebuf, e_sem.at[0])
        left_e = jnp.transpose(jnp.broadcast_to(ebuf[pl.ds(r // C, 1), :], (BS, BS)))
        rate = left_e + rates[pl.ds(q, 1), :]
        for side in range(2):
            with scope("w_op%d" % side):
                arrive(ops.at[side], ops_sem.at[side])
            for k in range(R):
                both = decode(ops[side, k], OP_MAX)
                mats[2 * side, k * SR:(k + 1) * SR] = both[:SR]
                mats[2 * side + 1, k * SR:(k + 1) * SR] = both[SR:]
        mid = dot3(mats[0], out[:, slot(q)], NN)
        mid = dot3(mid, mats[2], NT) / rate
        mid = dot3(mats[1], mid, NN)
        x = -dot3(mid, mats[3], NT)
        out[:, slot(q)] = x
        peak = jnp.max(jnp.abs(x), axis=0, keepdims=True) * 1.01 + 1e-30
        scale = peak.astype(BF16)
        xz[s, U, :PAD] = jnp.broadcast_to(scale, (PAD, BS))
        xz[s, U, PAD:] = encode(x, 1.0 / scale.astype(F32))

    def z_index(u, s):
        m = c + C * u
        j = jnp.where(d[s] - m <= m, d[s] - m, m)
        k = jnp.where(j == r, U, jnp.where(j % C == c, j // C, u))
        return j, k

    def collect(u, s, extra=True):
        j, k = z_index(u, s)
        landed = r < j
        if u >= U // 2:
            landed = landed & (j % C != c)
        landed = landed & extra

        for h in range(PARTS):
            block = xz.at[s, u, part(h)]

            @pl.when(landed)
            def _(block=block, h=h):
                arrive(block, xz_sem.at[s, u, h])

            send(landed & (r // 2 < j // 2) & (r % 2 != j % 2), block, block,
                 xz_sem.at[s, u, h], (r + 1 - 2 * (r % 2), c))

    def right(u, s):
        m = c + C * u

        def apply(a, dims):
            out[:, slot(u)] -= mm(own[0], a, dims) + mm(own[1], a, dims)

        def moved():
            arrive(atb.at[s, u], at_sem.at[s, u])

        if u >= U // 2:
            moved()
            apply(atb[s, u], NN)
            return
        if s == 0:
            @pl.when(m == r)
            def _():
                apply(upper[:, slot(u)], NT)

            @pl.when(m != r)
            def _():
                moved()
                apply(atb[s, u], NN)
        else:
            @pl.when(m == r)
            def _():
                apply(an[u], NT)

            @pl.when(m == r + 1)
            def _():
                moved()
                apply(atb[s, u], NT)

            @pl.when(m > r + 1)
            def _():
                moved()
                apply(atb[s, u], NN)

    def left(u, s):
        j, k = z_index(u, s)
        a = an[u] if s > 0 else upper[:, slot(u)]
        zh, zl = halves(decoded(s, k))

        def apply(dims):
            out[:, slot(u)] -= mm(a, zh, dims) + mm(a, zl, dims)

        low, high = C * u, C * u + C - 1
        if 2 * low >= d[s]:
            apply(NN)
        elif 2 * high < d[s]:
            apply(NT)
        else:
            m = c + C * u
            straight = d[s] - m <= m
            pl.when(straight)(lambda: apply(NN))
            pl.when(jnp.logical_not(straight))(lambda: apply(NT))

    def on_targets(s, fns, but=None):
        for u in range(U):
            live = target(r, c + C * u, s)
            if but is not None:
                live = live & jnp.logical_not(but(u))

            @pl.when(live)
            def _(u=u):
                for fn in fns:
                    fn(u, s)

    @pl.when(c == o[0])
    def _():
        with scope("solve0"):
            solve(0)

    with scope("give0"):
        give_row(0)
    with scope("take0"):
        take_row(0)
        split_own(0)
        send_upper(c == o[0])

    q1 = (d[1] - r) // C
    first = c == o[1]

    def picked(u):
        return first & (q1 == u)

    with scope("pick0"):
        for u in range(U // 2 - 1, U):
            collect(u, 0, picked(u))

            @pl.when(picked(u))
            def _(u=u):
                right(u, 0)
                left(u, 0)

    @pl.when(first)
    def _():
        with scope("solve1"):
            solve(1)

    with scope("give1"):
        give_row(1)
        send_upper(c == o[1])

    with scope("right0"):
        on_targets(0, (right,), picked)
    with scope("hand"):
        for u in range(U):
            hand_down(u)
    with scope("collect0"):
        for u in range(U):
            collect(u, 0, jnp.logical_not(picked(u)))
    with scope("left0"):
        on_targets(0, (left,), picked)

    with scope("take1"):
        take_row(1)
        split_own(1)
    with scope("w_an"):
        for u in range(U):
            @pl.when(target(r, c + C * u, 1))
            def _(u=u):
                arrive(an.at[u], an_sem.at[u])
    with scope("right1"):
        on_targets(1, (right,))
    with scope("collect1"):
        for u in range(U):
            collect(u, 1)
    with scope("left1"):
        on_targets(1, (left,))

    with scope("drain"):
        for cond, copy in sends:
            @pl.when(cond)
            def _(copy=copy):
                copy.wait_send()


def store(work, out, sem):
    lanes = work.shape[1] // out.shape[1]
    for j in range(out.shape[1]):
        pltpu.make_async_copy(work.at[:, pl.ds(j * lanes, lanes)], out.at[:, j, 0, :], sem.at[0]).start()
    pltpu.make_async_copy(work, work, sem.at[0]).wait()


def on_device(state, coupling, coupling_t, factor, cofactor, rates):
    R = lax.axis_size("row")
    C = lax.axis_size("col")
    U = 2 * R // C
    BS = state.shape[0]
    SR = factor.shape[2]
    flat = U * BS
    lanes = 128
    vmem = pl.BlockSpec(memory_space=pltpu.VMEM)
    hbm = pl.BlockSpec(memory_space=pltpu.HBM)
    dma = pltpu.SemaphoreType.DMA
    work = pl.pallas_call(
        functools.partial(kernel, R, C, U, BS, SR),
        out_shape=jax.ShapeDtypeStruct((BS, flat), F32),
        in_specs=[hbm] * 6,
        out_specs=vmem,
        scratch_shapes=[
            pltpu.VMEM((BS, flat), BF16),
            pltpu.VMEM((BS, flat), BF16),
            pltpu.VMEM((2, U, SR, BS), F32),
            pltpu.VMEM((U, BS), F32),
            pltpu.VMEM((U, 2 * SR, BS), BF16),
            pltpu.VMEM((2, R, 2 * SR, BS), BF16),
            pltpu.VMEM((4, BS, BS), F32),
            pltpu.VMEM((U, BS), F32),
            pltpu.VMEM((STEPS, U + 1, PAD + BS, BS), BF16),
            pltpu.VMEM((2, BS, BS), BF16),
            pltpu.VMEM((STEPS, U, BS, BS), BF16),
            pltpu.VMEM((U, BS, BS), BF16),
            dma((5,)),
            dma((2,)),
            dma((1,)),
            dma((STEPS, U + 1, PARTS)),
            dma((STEPS, U)),
            dma((U,)),
            dma((1,)),
        ],
        compiler_params=pltpu.CompilerParams(
            collective_id=0, has_side_effects=True, vmem_limit_bytes=VMEM_LIMIT),
    )(
        state.reshape(BS, flat // lanes, 1, lanes),
        coupling.reshape(BS, flat),
        coupling_t.reshape(coupling_t.shape[0], BS, flat),
        factor.reshape(U, SR, BS),
        cofactor.reshape(U, SR, BS),
        rates,
    )
    out = pl.pallas_call(
        store,
        out_shape=jax.ShapeDtypeStruct((BS, flat // lanes, 1, lanes), F32),
        in_specs=[vmem],
        out_specs=hbm,
        scratch_shapes=[dma((1,))],
        compiler_params=pltpu.CompilerParams(vmem_limit_bytes=2 * 1024 * 1024),
    )(work)
    return out.reshape(BS, 1, flat)


VMEM_LIMIT = 61 * 1024 * 1024


def solution(mesh):
    return jax.shard_map(
        on_device,
        mesh=mesh,
        in_specs=(
            P("row", "col", None),
            P("row", "col", None),
            P(None, "row", "col", None),
            P(None, "col", "row", None),
            P(None, "col", "row", None),
            P(None, "col", None),
        ),
        out_specs=P("row", "col", None),
        check_vma=False,
    )
```

```python
import functools

import jax
import jax.numpy as jnp
from jax import lax
from jax.experimental import pallas as pl
from jax.experimental.pallas import tpu as pltpu
from jax.sharding import PartitionSpec as P

STEPS = 2
PARTS = 2
PAD = 16
OP_MAX = 1.3
MESH = pl.DeviceIdType.MESH
F32 = jnp.float32
BF16 = jnp.bfloat16
NN = (((1,), (0,)), ((), ()))
NT = (((1,), (1,)), ((), ()))
scope = jax.named_scope


def halves(x):
    hi = x.astype(BF16)
    return hi, (x - hi.astype(F32)).astype(BF16)


def mm(a, b, dims):
    return lax.dot_general(a, b, dims, preferred_element_type=F32)


def dot3(a, b, dims):
    ah, al = halves(a)
    bh, bl = halves(b)
    return mm(ah, bh, dims) + (mm(ah, bl, dims) + mm(al, bh, dims))


def encode(x, inverse):
    v = jnp.exp2(jnp.sqrt(jnp.abs(x) * inverse) * 250.0 - 125.0)
    return jnp.where(x < 0, -v, v).astype(BF16)


def decode(v, scale):
    v = v.astype(F32)
    y = jnp.log2(jnp.abs(v)) * (1.0 / 250.0) + 0.5
    x = y * y * scale
    return jnp.where(v < 0, -x, x)


def kernel(R, C, U, BS, SR, state, upper_in, lower_in, factor, cofactor, rates_in, out,
           upper, lower, raw, rates, enc, ops, mats, ebuf, xz, own, atb, an,
           load_sem, ops_sem, e_sem, xz_sem, at_sem, an_sem, send_sem):
    H = R // 2
    r = lax.axis_index("row")
    c = lax.axis_index("col")
    d = [2 * R - 1 - s for s in range(STEPS)]

    def owner(row, s):
        return (d[s] - row) % C

    o = [owner(r, s) for s in range(STEPS)]
    sends = []
    me = r * C + c

    barrier = pltpu.get_barrier_semaphore()

    @pl.loop(1, R * C)
    def _(k):
        peer = (me + k) % (R * C)
        pl.semaphore_signal(barrier, inc=1, device_id=(peer // C, peer % C), device_id_type=MESH)

    pltpu.make_async_copy(cofactor, raw.at[0], load_sem.at[0]).start()
    pltpu.make_async_copy(factor, raw.at[1], load_sem.at[0]).start()
    pltpu.make_async_copy(rates_in.at[:, 0, :], rates, load_sem.at[1]).start()
    pltpu.make_async_copy(lower_in.at[0], lower, load_sem.at[2]).start()
    lanes = out.shape[1] // state.shape[1]
    for j in range(state.shape[1]):
        pltpu.make_async_copy(state.at[:, j, 0, :], out.at[:, pl.ds(j * lanes, lanes)], load_sem.at[3]).start()
    pltpu.make_async_copy(upper_in, upper, load_sem.at[4]).start()

    def arrive(ref, sem):
        pltpu.make_async_copy(ref, ref, sem).wait()

    def send(cond, src, dst, sem, dev):
        copy = pltpu.make_async_remote_copy(
            src_ref=src, dst_ref=dst, send_sem=send_sem.at[0], recv_sem=sem,
            device_id=dev, device_id_type=MESH)
        sends.append((cond, copy))

        @pl.when(cond)
        def _():
            copy.start()

    def send_or_local(cond, src, dst, sem, dev):
        mine = (dev[0] == r) & (dev[1] == c)
        send(cond & jnp.logical_not(mine), src, dst, sem, dev)

        @pl.when(cond & mine)
        def _():
            pltpu.make_async_copy(src, dst, sem).start()

    def slot(u):
        if isinstance(u, int):
            return pl.ds(u * BS, BS)
        return pl.ds(pl.multiple_of(u * BS, BS), BS)

    def target(row, m, s):
        return (row <= m) & (row + m < d[s])

    with scope("encode"):
        arrive(raw, load_sem.at[0])
        for u in range(U):
            both = jnp.concatenate([raw[0, u], raw[1, u]], axis=0)
            enc[u] = encode(both, 1.0 / OP_MAX)
        arrive(rates, load_sem.at[1])

    with scope("barrier"):
        pl.semaphore_wait(barrier, R * C - 1)

    def send_left():
        for u in range(U // 2):
            m = c + C * u
            send_or_local(m < R, enc.at[u], ops.at[0, r], ops_sem.at[0], (m, owner(m, 0)))

    def send_right(s):
        for u in range(U // 2 - s, U):
            to = d[s] - (c + C * u)
            send_or_local((to >= 0) & (to < R), enc.at[u], ops.at[1, r], ops_sem.at[1], (to, c))

    def send_lower(first):
        to = (r + H) % R
        top = (d[0] - 1 - to - c) // C
        for u in range(U - 1, -1, -1):
            m = c + C * u
            turn = u == top if first else u != top
            send(target(to, m, 0) & (m != to) & turn, lower.at[:, slot(u)], atb.at[0, u], at_sem.at[0, u], (to, c))

    early = (c >= 1) & (c != o[0]) & (c != o[1])
    lowest = (jnp.maximum(r + 1 - c, 0) + C - 1) // C

    def send_upper(cond):
        for u in range(U):
            m = c + C * u - 1
            to = (c + C - 1) % C
            to_u = jnp.maximum(jnp.where(c >= 1, u, u - 1), 0)
            send(cond(u) & (m >= 0) & target(r, m, 1), upper.at[:, slot(u)], an.at[to_u],
                 an_sem.at[to_u], (r, to))

    def hand_down(u):
        m = c + C * u
        live = (r >= 1) & (m >= r) & target(r - 1, m, 1)
        to = (jnp.maximum(r - 1, 0), c)
        if u < U // 2:
            send(live & (m == r), upper.at[:, slot(u)], atb.at[1, u], at_sem.at[1, u], to)
        send(live & (m != r), atb.at[0, u], atb.at[1, u], at_sem.at[1, u], to)

    with scope("sends0"):
        send_left()
        send_right(0)
        for s in range(STEPS):
            send_or_local(c == r % C, rates, ebuf, e_sem.at[0], (r, o[s]))
        arrive(lower, load_sem.at[2])
        send_lower(True)
        send_right(1)
        send_lower(False)
        arrive(upper, load_sem.at[4])
        arrive(out, load_sem.at[3])
        send_upper(lambda u: early & (u == lowest))

    half = BS // PARTS

    def part(h):
        if h == 0:
            return pl.ds(0, PAD + half)
        return pl.ds(PAD + h * half, half)

    def spread(s, h, who):
        own_col = r % C == c
        k = jnp.where(own_col, r // C, (d[s] - r) // C)
        has = (own_col | (c == o[s])) & who

        def give(cond, to):
            send(cond & has, xz.at[s, U, part(h)], xz.at[s, k, part(h)], xz_sem.at[s, k, h], (to, c))

        give(r % 2 == 1, jnp.maximum(r - 1, 0))
        for back in range(1, R // 2):
            pair = r // 2 - back
            give(pair >= 0, jnp.maximum(2 * pair + 1 - r % 2, 0))

    def give_row(s):
        at = c == o[s]
        far = (o[s] == 0) & at
        for h in range(PARTS):
            block = xz.at[s, U, part(h)]
            sem = xz_sem.at[s, U, h]
            if s == 0:
                send(far, block, block, sem, (r, C - 1))
                send(at & (o[s] >= 1), block, block, sem, (r, jnp.maximum(c - 1, 0)))
                spread(s, h, at)
                send(at & (o[s] <= C - 2), block, block, sem, (r, jnp.minimum(c + 1, C - 1)))
            else:
                send(at & (o[s] >= 2), block, block, sem, (r, jnp.maximum(c - 2, 0)))
                send(at & (o[s] <= C - 3), block, block, sem, (r, jnp.minimum(c + 2, C - 1)))
                spread(s, h, at)
                send(at & (o[s] >= 1), block, block, sem, (r, jnp.maximum(c - 1, 0)))
                send(at & (o[s] <= C - 2), block, block, sem, (r, jnp.minimum(c + 1, C - 1)))

    def take_row(s):
        other = c != o[s]
        near = 1 if s == 0 else 2
        down = (c <= o[s] - near) & (c >= 1)
        up = (c >= o[s] + near) & (c < C - 1)
        if s == 0:
            up = up & jnp.logical_not((o[s] == 0) & (c == C - 2))
        for h in range(PARTS):
            block = xz.at[s, U, part(h)]
            sem = xz_sem.at[s, U, h]

            @pl.when(other)
            def _(block=block, sem=sem):
                arrive(block, sem)

            send(down, block, block, sem, (r, jnp.maximum(c - 1, 0)))
            send(up, block, block, sem, (r, jnp.minimum(c + 1, C - 1)))
            spread(s, h, other)

    def decoded(s, k):
        return decode(xz[s, k, PAD:], xz[s, k, 0:1, :].astype(F32))

    def split_own(s):
        xh, xl = halves(decoded(s, U))
        own[0] = xh
        own[1] = xl

    def solve(s):
        q = (d[s] - r) // C
        with scope("w_e"):
            arrive(ebuf, e_sem.at[0])
        left_e = jnp.transpose(jnp.broadcast_to(ebuf[pl.ds(r // C, 1), :], (BS, BS)))
        rate = left_e + rates[pl.ds(q, 1), :]
        for side in range(2):
            with scope("w_op%d" % side):
                arrive(ops.at[side], ops_sem.at[side])
            if s == 0 and side == 0:
                pass_left.start()
            for k in range(R):
                both = decode(ops[side, k], OP_MAX)
                mats[2 * side, k * SR:(k + 1) * SR] = both[:SR]
                mats[2 * side + 1, k * SR:(k + 1) * SR] = both[SR:]
        mid = dot3(mats[0], out[:, slot(q)], NN)
        mid = dot3(mid, mats[2], NT) / rate
        mid = dot3(mats[1], mid, NN)
        x = -dot3(mid, mats[3], NT)
        out[:, slot(q)] = x
        peak = jnp.max(jnp.abs(x), axis=0, keepdims=True) * 1.01 + 1e-30
        scale = peak.astype(BF16)
        xz[s, U, :PAD] = jnp.broadcast_to(scale, (PAD, BS))
        xz[s, U, PAD:] = encode(x, 1.0 / scale.astype(F32))

    def z_index(u, s):
        m = c + C * u
        j = jnp.where(d[s] - m <= m, d[s] - m, m)
        k = jnp.where(j == r, U, jnp.where(j % C == c, j // C, u))
        return j, k

    def collect(u, s, extra=True):
        j, k = z_index(u, s)
        landed = r < j
        if u >= U // 2:
            landed = landed & (j % C != c)
        landed = landed & extra

        for h in range(PARTS):
            block = xz.at[s, u, part(h)]

            @pl.when(landed)
            def _(block=block, h=h):
                arrive(block, xz_sem.at[s, u, h])

            send(landed & (r // 2 < j // 2) & (r % 2 != j % 2), block, block,
                 xz_sem.at[s, u, h], (r + 1 - 2 * (r % 2), c))

    def right(u, s):
        m = c + C * u

        def apply(a, dims):
            out[:, slot(u)] -= mm(own[0], a, dims) + mm(own[1], a, dims)

        def moved():
            arrive(atb.at[s, u], at_sem.at[s, u])

        if u >= U // 2:
            moved()
            apply(atb[s, u], NN)
            return
        if s == 0:
            @pl.when(m == r)
            def _():
                apply(upper[:, slot(u)], NT)

            @pl.when(m != r)
            def _():
                moved()
                apply(atb[s, u], NN)
        else:
            @pl.when(m == r)
            def _():
                apply(an[u], NT)

            @pl.when(m == r + 1)
            def _():
                moved()
                apply(atb[s, u], NT)

            @pl.when(m > r + 1)
            def _():
                moved()
                apply(atb[s, u], NN)

    def left(u, s):
        j, k = z_index(u, s)
        a = an[u] if s > 0 else upper[:, slot(u)]
        zh, zl = halves(decoded(s, k))

        def apply(dims):
            out[:, slot(u)] -= mm(a, zh, dims) + mm(a, zl, dims)

        low, high = C * u, C * u + C - 1
        if 2 * low >= d[s]:
            apply(NN)
        elif 2 * high < d[s]:
            apply(NT)
        else:
            m = c + C * u
            straight = d[s] - m <= m
            pl.when(straight)(lambda: apply(NN))
            pl.when(jnp.logical_not(straight))(lambda: apply(NT))

    def on_targets(s, fns, but=None):
        for u in range(U):
            live = target(r, c + C * u, s)
            if but is not None:
                live = live & jnp.logical_not(but(u))

            @pl.when(live)
            def _(u=u):
                for fn in fns:
                    fn(u, s)

    pass_left = pltpu.make_async_remote_copy(
        src_ref=ops.at[0], dst_ref=ops.at[0], send_sem=send_sem.at[0], recv_sem=ops_sem.at[0],
        device_id=(r, o[1]), device_id_type=MESH)
    sends.append((c == o[0], pass_left))

    @pl.when(c == o[0])
    def _():
        with scope("solve0"):
            solve(0)

    with scope("give0"):
        give_row(0)
    with scope("take0"):
        take_row(0)
        split_own(0)
        send_upper(lambda u: (c != o[1]) & jnp.logical_not(early & (u == lowest)))

    q1 = (d[1] - r) // C
    first = c == o[1]

    def picked(u):
        return first & (q1 == u)

    with scope("pick0"):
        for u in range(U // 2 - 1, U):
            collect(u, 0, picked(u))

            @pl.when(picked(u))
            def _(u=u):
                right(u, 0)
                left(u, 0)

    @pl.when(first)
    def _():
        with scope("solve1"):
            solve(1)

    with scope("give1"):
        give_row(1)
        send_upper(lambda u: c == o[1])

    with scope("right0"):
        on_targets(0, (right,), picked)
    with scope("hand"):
        for u in range(U):
            hand_down(u)
    with scope("collect0"):
        for u in range(U):
            collect(u, 0, jnp.logical_not(picked(u)))
    with scope("left0"):
        on_targets(0, (left,), picked)

    with scope("take1"):
        take_row(1)
        split_own(1)
    with scope("w_an"):
        for u in range(U):
            @pl.when(target(r, c + C * u, 1))
            def _(u=u):
                arrive(an.at[u], an_sem.at[u])
    with scope("right1"):
        on_targets(1, (right,))
    for u in range(U):
        with scope("collect1_%d" % u):
            collect(u, 1)

        @pl.when(target(r, c + C * u, 1))
        def _(u=u):
            with scope("left1_%d" % u):
                left(u, 1)

    with scope("drain"):
        for cond, copy in sends:
            @pl.when(cond)
            def _(copy=copy):
                copy.wait_send()


def store(work, out, sem):
    lanes = work.shape[1] // out.shape[1]
    for j in range(out.shape[1]):
        pltpu.make_async_copy(work.at[:, pl.ds(j * lanes, lanes)], out.at[:, j, 0, :], sem.at[0]).start()
    pltpu.make_async_copy(work, work, sem.at[0]).wait()


def on_device(state, coupling, coupling_t, factor, cofactor, rates):
    R = lax.axis_size("row")
    C = lax.axis_size("col")
    U = 2 * R // C
    BS = state.shape[0]
    SR = factor.shape[2]
    flat = U * BS
    lanes = 128
    vmem = pl.BlockSpec(memory_space=pltpu.VMEM)
    hbm = pl.BlockSpec(memory_space=pltpu.HBM)
    dma = pltpu.SemaphoreType.DMA
    work = pl.pallas_call(
        functools.partial(kernel, R, C, U, BS, SR),
        out_shape=pltpu.VMEM((BS, flat), F32),
        in_specs=[hbm] * 6,
        out_specs=vmem,
        scratch_shapes=[
            pltpu.VMEM((BS, flat), BF16),
            pltpu.VMEM((BS, flat), BF16),
            pltpu.VMEM((2, U, SR, BS), F32),
            pltpu.VMEM((U, BS), F32),
            pltpu.VMEM((U, 2 * SR, BS), BF16),
            pltpu.VMEM((2, R, 2 * SR, BS), BF16),
            pltpu.VMEM((4, BS, BS), F32),
            pltpu.VMEM((U, BS), F32),
            pltpu.VMEM((STEPS, U + 1, PAD + BS, BS), BF16),
            pltpu.VMEM((2, BS, BS), BF16),
            pltpu.VMEM((STEPS, U, BS, BS), BF16),
            pltpu.VMEM((U, BS, BS), BF16),
            dma((5,)),
            dma((2,)),
            dma((1,)),
            dma((STEPS, U + 1, PARTS)),
            dma((STEPS, U)),
            dma((U,)),
            dma((1,)),
        ],
        compiler_params=pltpu.CompilerParams(
            collective_id=0, has_side_effects=True, vmem_limit_bytes=VMEM_LIMIT),
    )(
        state.reshape(BS, flat // lanes, 1, lanes),
        coupling.reshape(BS, flat),
        coupling_t.reshape(coupling_t.shape[0], BS, flat),
        factor.reshape(U, SR, BS),
        cofactor.reshape(U, SR, BS),
        rates,
    )
    out = pl.pallas_call(
        store,
        out_shape=jax.ShapeDtypeStruct((BS, flat // lanes, 1, lanes), F32),
        in_specs=[vmem],
        out_specs=hbm,
        scratch_shapes=[dma((1,))],
        compiler_params=pltpu.CompilerParams(vmem_limit_bytes=2 * 1024 * 1024),
    )(work)
    return out.reshape(BS, 1, flat)


VMEM_LIMIT = 61 * 1024 * 1024


def solution(mesh):
    return jax.shard_map(
        on_device,
        mesh=mesh,
        in_specs=(
            P("row", "col", None),
            P("row", "col", None),
            P(None, "row", "col", None),
            P(None, "col", "row", None),
            P(None, "col", "row", None),
            P(None, "col", None),
        ),
        out_specs=P("row", "col", None),
        check_vma=False,
    )
```

```python
import functools

import jax
import jax.numpy as jnp
from jax import lax
from jax.experimental import pallas as pl
from jax.experimental.pallas import tpu as pltpu
from jax.sharding import PartitionSpec as P

STEPS = 2
PARTS = 2
PAD = 16
SAME = False
OP_MAX = 1.3
MESH = pl.DeviceIdType.MESH
F32 = jnp.float32
BF16 = jnp.bfloat16
NN = (((1,), (0,)), ((), ()))
NT = (((1,), (1,)), ((), ()))
scope = jax.named_scope


def halves(x):
    hi = x.astype(BF16)
    return hi, (x - hi.astype(F32)).astype(BF16)


def mm(a, b, dims):
    return lax.dot_general(a, b, dims, preferred_element_type=F32)


def dot3(a, b, dims):
    return mm(a[0], b[0], dims) + (mm(a[0], b[1], dims) + mm(a[1], b[0], dims))


def encode(x, inverse):
    v = jnp.exp2(jnp.sqrt(jnp.abs(x) * inverse) * 250.0 - 125.0)
    return jnp.where(x < 0, -v, v).astype(BF16)


def decode(v, scale):
    v = v.astype(F32)
    y = jnp.log2(jnp.abs(v)) * (1.0 / 250.0) + 0.5
    x = y * y * scale
    return jnp.where(v < 0, -x, x)


def kernel(R, C, U, BS, SR, state, upper_in, lower_in, factor, cofactor, rates_in, out,
           upper, lower, turned, raw, rates, enc, ops, mats, ebuf, xz, own, atb, an,
           load_sem, ops_sem, e_sem, xz_sem, at_sem, an_sem, send_sem):
    H = R // 2
    r = lax.axis_index("row")
    c = lax.axis_index("col")
    d = [2 * R - 1 - s for s in range(STEPS)]

    def owner(row, s):
        return (d[s] - row) % C

    o = [owner(r, s) for s in range(STEPS)]
    sends = []
    me = r * C + c

    barrier = pltpu.get_barrier_semaphore()

    @pl.loop(1, R * C)
    def _(k):
        peer = (me + k) % (R * C)
        pl.semaphore_signal(barrier, inc=1, device_id=(peer // C, peer % C), device_id_type=MESH)

    pltpu.make_async_copy(cofactor, raw.at[0], load_sem.at[0]).start()
    pltpu.make_async_copy(factor, raw.at[1], load_sem.at[0]).start()
    pltpu.make_async_copy(rates_in.at[:, 0, :], rates, load_sem.at[1]).start()
    pltpu.make_async_copy(lower_in, lower, load_sem.at[2]).start()
    lanes = out.shape[1] // state.shape[1]
    for j in range(state.shape[1]):
        pltpu.make_async_copy(state.at[:, j, 0, :], out.at[:, pl.ds(j * lanes, lanes)], load_sem.at[3]).start()
    pltpu.make_async_copy(upper_in, upper, load_sem.at[4]).start()

    def arrive(ref, sem):
        pltpu.make_async_copy(ref, ref, sem).wait()

    def send(cond, src, dst, sem, dev):
        copy = pltpu.make_async_remote_copy(
            src_ref=src, dst_ref=dst, send_sem=send_sem.at[0], recv_sem=sem,
            device_id=dev, device_id_type=MESH)
        sends.append((cond, copy))

        @pl.when(cond)
        def _():
            copy.start()

    def send_or_local(cond, src, dst, sem, dev):
        mine = (dev[0] == r) & (dev[1] == c)
        send(cond & jnp.logical_not(mine), src, dst, sem, dev)

        @pl.when(cond & mine)
        def _():
            pltpu.make_async_copy(src, dst, sem).start()

    def slot(u):
        if isinstance(u, int):
            return pl.ds(u * BS, BS)
        return pl.ds(pl.multiple_of(u * BS, BS), BS)

    def target(row, m, s):
        return (row <= m) & (row + m < d[s])

    with scope("encode"):
        arrive(raw, load_sem.at[0])
        for u in range(U):
            both = jnp.concatenate([raw[0, u], raw[1, u]], axis=0)
            enc[u] = encode(both, 1.0 / OP_MAX)
        arrive(rates, load_sem.at[1])

    with scope("barrier"):
        pl.semaphore_wait(barrier, R * C - 1)

    def send_left(s):
        for u in range(U // 2):
            m = c + C * u
            send_or_local(m < R, enc.at[u], ops.at[0, r], ops_sem.at[0], (m, owner(m, s)))

    def send_right(s):
        for u in range(U // 2 - s, U):
            to = d[s] - (c + C * u)
            send_or_local((to >= 0) & (to < R), enc.at[u], ops.at[1, r], ops_sem.at[1], (to, c))

    def send_lower(first):
        to = (r + H) % R
        top = (d[0] - 1 - to - c) // C
        for u in range(U - 1, -1, -1):
            m = c + C * u
            turn = u == top if first else u != top
            send(target(to, m, 0) & (m != to) & turn, lower.at[0, :, slot(u)], atb.at[0, u], at_sem.at[0, u], (to, c))

    q1 = (d[1] - r) // C
    first = c == o[1]
    top = (d[0] - 1 - r - c) // C
    ahead = c != o[0]

    def needs(u):
        m = c + C * u
        return target(r, m, 0) & (m != r)

    def picked(u):
        return first & (q1 == u)

    def crossing(i, m):
        return (m % C == C - 1) | ((m - i) % C == 0 if SAME else False)

    def send_turned(cond):
        for t in range(2):
            m = (r + H) % R + R * t - 1
            for u in range(U // 2):
                i = c + C * u
                live = cond & (m >= 0) & target(i, m, 1) & crossing(i, m)
                to_u = jnp.clip(m // C, 0, U - 1)
                mine = (i == r) & (m % C == c)
                k = t * (U // 2) + u

                @pl.when(live)
                def _(t=t, u=u, k=k):
                    turned[k] = jnp.transpose(lower[t, :, slot(u)])

                send(live & jnp.logical_not(mine), turned.at[k], an.at[to_u], an_sem.at[to_u], (i, m % C))

                @pl.when(live & mine)
                def _(k=k, to_u=to_u):
                    pltpu.make_async_copy(turned.at[k], an.at[to_u], an_sem.at[to_u]).start()

    def send_upper(cond):
        for u in range(U):
            m = c + C * u - 1
            to = (c + C - 1) % C
            to_u = jnp.maximum(jnp.where(c >= 1, u, u - 1), 0)
            send(cond & jnp.logical_not(crossing(r, m)) & (m >= 0) & target(r, m, 1), upper.at[:, slot(u)], an.at[to_u],
                 an_sem.at[to_u], (r, to))

    def hand_down(u):
        m = c + C * u
        live = (r >= 1) & (m >= r) & target(r - 1, m, 1)
        to = (jnp.maximum(r - 1, 0), c)
        if u < U // 2:
            send(live & (m == r), upper.at[:, slot(u)], atb.at[1, u], at_sem.at[1, u], to)
        send(live & (m != r), atb.at[0, u], atb.at[1, u], at_sem.at[1, u], to)

    with scope("sends0"):
        send_left(0)
        send_right(0)
        for s in range(STEPS):
            send_or_local(c == r % C, rates, ebuf, e_sem.at[0], (r, o[s]))
        send_left(1)
        arrive(lower, load_sem.at[2])
        send_lower(True)
        send_right(1)
        send_lower(False)
        arrive(upper, load_sem.at[4])
        arrive(out, load_sem.at[3])
        send_upper(c != o[0])

    with scope("gate"):
        @pl.when(ahead & needs(top))
        def _():
            arrive(atb.at[0, top], at_sem.at[0, top])

        send_turned(c != o[0])

    half = BS // PARTS

    def part(h):
        if h == 0:
            return pl.ds(0, PAD + half)
        return pl.ds(PAD + h * half, half)

    def spread(s, h, who):
        own_col = r % C == c
        k = jnp.where(own_col, r // C, (d[s] - r) // C)
        has = (own_col | (c == o[s])) & who

        def give(cond, to):
            send(cond & has, xz.at[s, U, part(h)], xz.at[s, k, part(h)], xz_sem.at[s, k, h], (to, c))

        give(r % 2 == 1, jnp.maximum(r - 1, 0))
        for back in range(1, R // 2):
            pair = r // 2 - back
            give(pair >= 0, jnp.maximum(2 * pair + 1 - r % 2, 0))

    def give_row(s):
        at = c == o[s]
        goal = (o[s] + C - 1) % C
        for h in range(PARTS):
            block = xz.at[s, U, part(h)]
            sem = xz_sem.at[s, U, h]
            if s == 0:
                send(at, block, block, sem, (r, goal))
                spread(s, h, at)
            for far_by in range(C - 1, 0, -1):
                for to in (c - far_by, c + far_by):
                    live = at & (to >= 0) & (to < C)
                    if s == 0:
                        live = live & (to != goal)
                    send(live, block, block, sem, (r, jnp.clip(to, 0, C - 1)))
                if far_by == 2 and s == 1:
                    spread(s, h, at)

    def take_row(s):
        other = c != o[s]
        for h in range(PARTS):
            block = xz.at[s, U, part(h)]
            sem = xz_sem.at[s, U, h]

            @pl.when(other)
            def _(block=block, sem=sem):
                arrive(block, sem)

            spread(s, h, other)

    def decoded(s, k):
        return decode(xz[s, k, PAD:], xz[s, k, 0:1, :].astype(F32))

    def split_own(s):
        xh, xl = halves(decoded(s, U))
        own[0] = xh
        own[1] = xl

    def prepare():
        with scope("w_e"):
            arrive(ebuf, e_sem.at[0])
        group = max(1, 16 // SR)
        for side in range(2):
            with scope("w_op%d" % side):
                arrive(ops.at[side], ops_sem.at[side])
            for k in range(0, R, group):
                both = [decode(ops[side, k + i], OP_MAX) for i in range(group)]
                for which in range(2):
                    rows = [b[which * SR:(which + 1) * SR] for b in both]
                    hi, lo = halves(rows[0] if group == 1 else jnp.concatenate(rows, axis=0))
                    mats[2 * side + which, 0, k * SR:(k + group) * SR] = hi
                    mats[2 * side + which, 1, k * SR:(k + group) * SR] = lo

    def solve(s):
        q = (d[s] - r) // C
        left_e = jnp.transpose(jnp.broadcast_to(ebuf[pl.ds(r // C, 1), :], (BS, BS)))
        rate = left_e + rates[pl.ds(q, 1), :]
        mat = [(mats[k, 0], mats[k, 1]) for k in range(4)]
        mid = dot3(mat[0], halves(out[:, slot(q)]), NN)
        mid = dot3(halves(mid), mat[2], NT) / rate
        mid = dot3(mat[1], halves(mid), NN)
        x = -dot3(halves(mid), mat[3], NT)
        out[:, slot(q)] = x
        peak = jnp.max(jnp.abs(x), axis=0, keepdims=True) * 1.01 + 1e-30
        scale = peak.astype(BF16)
        xz[s, U, :PAD] = jnp.broadcast_to(scale, (PAD, BS))
        xz[s, U, PAD:] = encode(x, 1.0 / scale.astype(F32))

    def z_index(u, s):
        m = c + C * u
        j = jnp.where(d[s] - m <= m, d[s] - m, m)
        k = jnp.where(j == r, U, jnp.where(j % C == c, j // C, u))
        return j, k

    def collect(u, s, extra=True):
        j, k = z_index(u, s)
        landed = r < j
        if u >= U // 2:
            landed = landed & (j % C != c)
        landed = landed & extra

        for h in range(PARTS):
            block = xz.at[s, u, part(h)]

            @pl.when(landed)
            def _(block=block, h=h):
                arrive(block, xz_sem.at[s, u, h])

            send(landed & (r // 2 < j // 2) & (r % 2 != j % 2), block, block,
                 xz_sem.at[s, u, h], (r + 1 - 2 * (r % 2), c))

    def right(u, s):
        m = c + C * u

        def apply(a, dims):
            out[:, slot(u)] -= mm(own[0], a, dims) + mm(own[1], a, dims)

        def moved():
            if s > 0:
                arrive(atb.at[s, u], at_sem.at[s, u])

        if u >= U // 2:
            moved()
            apply(atb[s, u], NN)
            return
        if s == 0:
            @pl.when(m == r)
            def _():
                apply(upper[:, slot(u)], NT)

            @pl.when(m != r)
            def _():
                moved()
                apply(atb[s, u], NN)
        else:
            @pl.when(m == r)
            def _():
                apply(an[u], NT)

            @pl.when(m == r + 1)
            def _():
                moved()
                apply(atb[s, u], NT)

            @pl.when(m > r + 1)
            def _():
                moved()
                apply(atb[s, u], NN)

    def left(u, s):
        j, k = z_index(u, s)
        a = an[u] if s > 0 else upper[:, slot(u)]
        zh, zl = halves(decoded(s, k))

        def apply(dims):
            out[:, slot(u)] -= mm(a, zh, dims) + mm(a, zl, dims)

        low, high = C * u, C * u + C - 1
        if 2 * low >= d[s]:
            apply(NN)
        elif 2 * high < d[s]:
            apply(NT)
        else:
            m = c + C * u
            straight = d[s] - m <= m
            pl.when(straight)(lambda: apply(NN))
            pl.when(jnp.logical_not(straight))(lambda: apply(NT))

    def on_targets(s, fns, but=None):
        for u in range(U):
            live = target(r, c + C * u, s)
            if but is not None:
                live = live & jnp.logical_not(but(u))

            @pl.when(live)
            def _(u=u):
                for fn in fns:
                    fn(u, s)

    @pl.when(c == o[0])
    def _():
        with scope("solve0"):
            prepare()
            solve(0)

    with scope("give0"):
        give_row(0)
        send_upper(c == o[0])
        send_turned(c == o[0])

    @pl.when(first)
    def _():
        with scope("prep"):
            prepare()

    with scope("take0"):
        take_row(0)
        split_own(0)

    with scope("pick0"):
        for u in range(U // 2 - 1, U):
            collect(u, 0, picked(u))

            @pl.when(picked(u))
            def _(u=u):
                right(u, 0)
                left(u, 0)

    @pl.when(first)
    def _():
        with scope("solve1"):
            solve(1)

    with scope("give1"):
        give_row(1)

    with scope("hand"):
        for u in range(U):
            @pl.when(needs(u) & jnp.logical_not(ahead & (top == u)))
            def _(u=u):
                arrive(atb.at[0, u], at_sem.at[0, u])

            hand_down(u)
    with scope("right0"):
        on_targets(0, (right,), picked)
    with scope("collect0"):
        for u in range(U):
            collect(u, 0, jnp.logical_not(picked(u)))
    with scope("left0"):
        on_targets(0, (left,), picked)

    with scope("take1"):
        take_row(1)
        split_own(1)
    with scope("w_an"):
        for u in range(U):
            @pl.when(target(r, c + C * u, 1))
            def _(u=u):
                arrive(an.at[u], an_sem.at[u])
    with scope("right1"):
        on_targets(1, (right,))
    for u in range(U):
        with scope("collect1_%d" % u):
            collect(u, 1)

        @pl.when(target(r, c + C * u, 1))
        def _(u=u):
            with scope("left1_%d" % u):
                left(u, 1)

    with scope("drain"):
        for cond, copy in sends:
            @pl.when(cond)
            def _(copy=copy):
                copy.wait_send()


def store(work, out, sem):
    lanes = work.shape[1] // out.shape[1]
    for j in range(out.shape[1]):
        pltpu.make_async_copy(work.at[:, pl.ds(j * lanes, lanes)], out.at[:, j, 0, :], sem.at[0]).start()
    pltpu.make_async_copy(work, work, sem.at[0]).wait()


def on_device(state, coupling, coupling_t, factor, cofactor, rates):
    R = lax.axis_size("row")
    C = lax.axis_size("col")
    U = 2 * R // C
    BS = state.shape[0]
    SR = factor.shape[2]
    flat = U * BS
    lanes = 128
    vmem = pl.BlockSpec(memory_space=pltpu.VMEM)
    hbm = pl.BlockSpec(memory_space=pltpu.HBM)
    dma = pltpu.SemaphoreType.DMA
    work = pl.pallas_call(
        functools.partial(kernel, R, C, U, BS, SR),
        out_shape=pltpu.VMEM((BS, flat), F32),
        in_specs=[hbm] * 6,
        out_specs=vmem,
        scratch_shapes=[
            pltpu.VMEM((BS, flat), BF16),
            pltpu.VMEM((2, BS, flat), BF16),
            pltpu.VMEM((U, BS, BS), BF16),
            pltpu.VMEM((2, U, SR, BS), F32),
            pltpu.VMEM((U, BS), F32),
            pltpu.VMEM((U, 2 * SR, BS), BF16),
            pltpu.VMEM((2, R, 2 * SR, BS), BF16),
            pltpu.VMEM((4, 2, BS, BS), BF16),
            pltpu.VMEM((U, BS), F32),
            pltpu.VMEM((STEPS, U + 1, PAD + BS, BS), BF16),
            pltpu.VMEM((2, BS, BS), BF16),
            pltpu.VMEM((STEPS, U, BS, BS), BF16),
            pltpu.VMEM((U, BS, BS), BF16),
            dma((5,)),
            dma((2,)),
            dma((1,)),
            dma((STEPS, U + 1, PARTS)),
            dma((STEPS, U)),
            dma((U,)),
            dma((1,)),
        ],
        compiler_params=pltpu.CompilerParams(
            collective_id=0, has_side_effects=True, vmem_limit_bytes=VMEM_LIMIT),
    )(
        state.reshape(BS, flat // lanes, 1, lanes),
        coupling.reshape(BS, flat),
        coupling_t.reshape(coupling_t.shape[0], BS, flat),
        factor.reshape(U, SR, BS),
        cofactor.reshape(U, SR, BS),
        rates,
    )
    out = pl.pallas_call(
        store,
        out_shape=jax.ShapeDtypeStruct((BS, flat // lanes, 1, lanes), F32),
        in_specs=[vmem],
        out_specs=hbm,
        scratch_shapes=[dma((1,))],
        compiler_params=pltpu.CompilerParams(vmem_limit_bytes=2 * 1024 * 1024),
    )(work)
    return out.reshape(BS, 1, flat)


VMEM_LIMIT = 61 * 1024 * 1024


def solution(mesh):
    return jax.shard_map(
        on_device,
        mesh=mesh,
        in_specs=(
            P("row", "col", None),
            P("row", "col", None),
            P(None, "row", "col", None),
            P(None, "col", "row", None),
            P(None, "col", "row", None),
            P(None, "col", None),
        ),
        out_specs=P("row", "col", None),
        check_vma=False,
    )
```

```python
import functools

import jax
import jax.numpy as jnp
from jax import lax
from jax.experimental import pallas as pl
from jax.experimental.pallas import tpu as pltpu
from jax.sharding import PartitionSpec as P

STEPS = 2
PARTS = 2
PAD = 16
SAME = True
OP_MAX = 1.3
MESH = pl.DeviceIdType.MESH
F32 = jnp.float32
BF16 = jnp.bfloat16
NN = (((1,), (0,)), ((), ()))
NT = (((1,), (1,)), ((), ()))
scope = jax.named_scope


def halves(x):
    hi = x.astype(BF16)
    return hi, (x - hi.astype(F32)).astype(BF16)


def mm(a, b, dims):
    return lax.dot_general(a, b, dims, preferred_element_type=F32)


def dot3(a, b, dims):
    return mm(a[0], b[0], dims) + (mm(a[0], b[1], dims) + mm(a[1], b[0], dims))


def encode(x, inverse):
    v = jnp.exp2(jnp.sqrt(jnp.abs(x) * inverse) * 250.0 - 125.0)
    return jnp.where(x < 0, -v, v).astype(BF16)


def decode(v, scale):
    v = v.astype(F32)
    y = jnp.log2(jnp.abs(v)) * (1.0 / 250.0) + 0.5
    x = y * y * scale
    return jnp.where(v < 0, -x, x)


def kernel(R, C, U, BS, SR, state, upper_in, lower_in, factor, cofactor, rates_in, out,
           upper, lower, turned, raw, rates, enc, ops, mats, ebuf, xz, own, atb, an,
           load_sem, ops_sem, e_sem, xz_sem, at_sem, an_sem, send_sem):
    H = R // 2
    r = lax.axis_index("row")
    c = lax.axis_index("col")
    d = [2 * R - 1 - s for s in range(STEPS)]

    def owner(row, s):
        return (d[s] - row) % C

    o = [owner(r, s) for s in range(STEPS)]
    sends = []
    me = r * C + c

    barrier = pltpu.get_barrier_semaphore()

    @pl.loop(1, R * C)
    def _(k):
        peer = (me + k) % (R * C)
        pl.semaphore_signal(barrier, inc=1, device_id=(peer // C, peer % C), device_id_type=MESH)

    pltpu.make_async_copy(cofactor, raw.at[0], load_sem.at[0]).start()
    pltpu.make_async_copy(factor, raw.at[1], load_sem.at[0]).start()
    pltpu.make_async_copy(rates_in.at[:, 0, :], rates, load_sem.at[1]).start()
    pltpu.make_async_copy(lower_in, lower, load_sem.at[2]).start()
    lanes = out.shape[1] // state.shape[1]
    for j in range(state.shape[1]):
        pltpu.make_async_copy(state.at[:, j, 0, :], out.at[:, pl.ds(j * lanes, lanes)], load_sem.at[3]).start()
    pltpu.make_async_copy(upper_in, upper, load_sem.at[4]).start()

    def arrive(ref, sem):
        pltpu.make_async_copy(ref, ref, sem).wait()

    def send(cond, src, dst, sem, dev):
        copy = pltpu.make_async_remote_copy(
            src_ref=src, dst_ref=dst, send_sem=send_sem.at[0], recv_sem=sem,
            device_id=dev, device_id_type=MESH)
        sends.append((cond, copy))

        @pl.when(cond)
        def _():
            copy.start()

    def send_or_local(cond, src, dst, sem, dev):
        mine = (dev[0] == r) & (dev[1] == c)
        send(cond & jnp.logical_not(mine), src, dst, sem, dev)

        @pl.when(cond & mine)
        def _():
            pltpu.make_async_copy(src, dst, sem).start()

    def slot(u):
        if isinstance(u, int):
            return pl.ds(u * BS, BS)
        return pl.ds(pl.multiple_of(u * BS, BS), BS)

    def target(row, m, s):
        return (row <= m) & (row + m < d[s])

    with scope("encode"):
        arrive(raw, load_sem.at[0])
        for u in range(U):
            both = jnp.concatenate([raw[0, u], raw[1, u]], axis=0)
            enc[u] = encode(both, 1.0 / OP_MAX)
        arrive(rates, load_sem.at[1])

    with scope("barrier"):
        pl.semaphore_wait(barrier, R * C - 1)

    def send_left(s):
        for u in range(U // 2):
            m = c + C * u
            send_or_local(m < R, enc.at[u], ops.at[0, r], ops_sem.at[0], (m, owner(m, s)))

    def send_right(s):
        for u in range(U // 2 - s, U):
            to = d[s] - (c + C * u)
            live = (to >= 0) & (to < R)
            if s > 0:
                live = live & (to % 2 == 1)
            send_or_local(live, enc.at[u], ops.at[1, r], ops_sem.at[1], (to, c))

    def send_lower(first):
        to = (r + H) % R
        top = (d[0] - 1 - to - c) // C
        for u in range(U - 1, -1, -1):
            m = c + C * u
            turn = u == top if first else u != top
            send(target(to, m, 0) & (m != to) & turn, lower.at[0, :, slot(u)], atb.at[0, u], at_sem.at[0, u], (to, c))

    def send_middle():
        for u in range(U):
            m = c + C * u
            send((r == 0) & (m >= H) & target(H - 1, m, 1), lower.at[0, :, slot(u)], atb.at[1, u],
                 at_sem.at[1, u], (H - 1, c))

    q1 = (d[1] - r) // C
    first = c == o[1]
    top = (d[0] - 1 - r - c) // C
    ahead = c != o[0]

    def needs(u):
        m = c + C * u
        return target(r, m, 0) & (m != r)

    def picked(u):
        return first & (q1 == u)

    def crossing(i, m):
        return (m % C == C - 1) | ((m - i) % C == 0 if SAME else False)

    def send_turned(cond):
        for t in range(2):
            m = (r + H) % R + R * t - 1
            for u in range(U // 2):
                i = c + C * u
                live = cond & (m >= 0) & target(i, m, 1) & crossing(i, m)
                to_u = jnp.clip(m // C, 0, U - 1)
                mine = (i == r) & (m % C == c)
                k = t * (U // 2) + u

                @pl.when(live)
                def _(t=t, u=u, k=k):
                    turned[k] = jnp.transpose(lower[t, :, slot(u)])

                send(live & jnp.logical_not(mine), turned.at[k], an.at[to_u], an_sem.at[to_u], (i, m % C))

                @pl.when(live & mine)
                def _(k=k, to_u=to_u):
                    pltpu.make_async_copy(turned.at[k], an.at[to_u], an_sem.at[to_u]).start()

    def send_upper(cond, held=None):
        late = first & (r % 2 == 0)
        for u in range(U):
            m = c + C * u - 1
            to = (c + C - 1) % C
            to_u = jnp.maximum(jnp.where(c >= 1, u, u - 1), 0)
            if u >= U // 2:
                now = late if held else cond & jnp.logical_not(late)
            elif held:
                continue
            else:
                now = cond
            send(now & jnp.logical_not(crossing(r, m)) & (m >= 0) & target(r, m, 1), upper.at[:, slot(u)], an.at[to_u],
                 an_sem.at[to_u], (r, to))

    def hand_down(u, rows):
        m = c + C * u
        live = rows & (r >= 1) & (r != H) & (m >= r) & target(r - 1, m, 1)
        to = (jnp.maximum(r - 1, 0), c)
        if u < U // 2:
            send(live & (m == r), upper.at[:, slot(u)], atb.at[1, u], at_sem.at[1, u], to)
        send(live & (m != r), atb.at[0, u], atb.at[1, u], at_sem.at[1, u], to)

    with scope("sends0"):
        send_left(0)
        send_right(0)
        for s in range(STEPS):
            send_or_local(c == r % C, rates, ebuf, e_sem.at[0], (r, o[s]))
        send_left(1)
        arrive(lower, load_sem.at[2])
        send_lower(True)
        send_right(1)
        send_lower(False)
        send_middle()
        arrive(upper, load_sem.at[4])
        arrive(out, load_sem.at[3])
        send_upper(c != o[0])

    with scope("gate"):
        @pl.when(ahead & needs(top))
        def _():
            arrive(atb.at[0, top], at_sem.at[0, top])

        send_turned(c != o[0])

    half = BS // PARTS

    def part(h):
        if h == 0:
            return pl.ds(0, PAD + half)
        return pl.ds(PAD + h * half, half)

    def spread(s, h, who):
        own_col = r % C == c
        k = jnp.where(own_col, r // C, (d[s] - r) // C)
        has = (own_col | (c == o[s])) & who

        def give(cond, to):
            send(cond & has, xz.at[s, U, part(h)], xz.at[s, k, part(h)], xz_sem.at[s, k, h], (to, c))

        give(r % 2 == 1, jnp.maximum(r - 1, 0))
        for back in range(1, R // 2):
            pair = r // 2 - back
            give(pair >= 0, jnp.maximum(2 * pair + 1 - r % 2, 0))

    def wants(col, s):
        return (col - r) % C < d[s] - 2 * r

    def give_row(s):
        at = c == o[s]
        home = r % C
        goal = (o[s] + C - 1) % C
        def give(cond, to):
            for h in range(PARTS):
                block = xz.at[s, U, part(h)]
                send(at & cond, block, block, xz_sem.at[s, U, h], (r, jnp.clip(to, 0, C - 1)))

        if s == 0:
            give(True, goal)
        else:
            give(home != c, home)
        for h in range(PARTS):
            spread(s, h, at)
        if s == 0:
            give((home != goal) & (home != c), home)
        for far_by in range(C - 1, 0, -1):
            for to in (c - far_by, c + far_by):
                live = (to >= 0) & (to < C) & (to != home) & wants(to, s)
                if s == 0:
                    live = live & (to != goal)
                give(live, to)

    def take_row(s):
        other = (c != o[s]) & (wants(c, s) | (c == r % C))
        if s == 0:
            other = other | first
        for h in range(PARTS):
            block = xz.at[s, U, part(h)]
            sem = xz_sem.at[s, U, h]

            @pl.when(other)
            def _(block=block, sem=sem):
                arrive(block, sem)

            spread(s, h, other)

    def decoded(s, k):
        return decode(xz[s, k, PAD:], xz[s, k, 0:1, :].astype(F32))

    def split_own(s):
        xh, xl = halves(decoded(s, U))
        own[s, 0] = xh
        own[s, 1] = xl

    def prepare(s):
        with scope("w_e"):
            arrive(ebuf, e_sem.at[0])
        group = max(1, 16 // SR)
        for side in range(2):
            with scope("w_op%d" % side):
                arrive(ops.at[side], ops_sem.at[side])
            if s == 0 and side == 1:
                pl.when(r % 2 == 1)(hand_right.start)
            for k in range(0, R, group):
                both = [decode(ops[side, k + i], OP_MAX) for i in range(group)]
                for which in range(2):
                    rows = [b[which * SR:(which + 1) * SR] for b in both]
                    hi, lo = halves(rows[0] if group == 1 else jnp.concatenate(rows, axis=0))
                    mats[2 * side + which, 0, k * SR:(k + group) * SR] = hi
                    mats[2 * side + which, 1, k * SR:(k + group) * SR] = lo

    def solve(s):
        q = (d[s] - r) // C
        left_e = jnp.transpose(jnp.broadcast_to(ebuf[pl.ds(r // C, 1), :], (BS, BS)))
        rate = left_e + rates[pl.ds(q, 1), :]
        mat = [(mats[k, 0], mats[k, 1]) for k in range(4)]
        mid = dot3(mat[0], halves(out[:, slot(q)]), NN)
        mid = dot3(halves(mid), mat[2], NT) / rate
        mid = dot3(mat[1], halves(mid), NN)
        x = -dot3(halves(mid), mat[3], NT)
        out[:, slot(q)] = x
        peak = jnp.max(jnp.abs(x), axis=0, keepdims=True) * 1.01 + 1e-30
        scale = peak.astype(BF16)
        xz[s, U, :PAD] = jnp.broadcast_to(scale, (PAD, BS))
        xz[s, U, PAD:] = encode(x, 1.0 / scale.astype(F32))

    def z_index(u, s):
        m = c + C * u
        j = jnp.where(d[s] - m <= m, d[s] - m, m)
        k = jnp.where(j == r, U, jnp.where(j % C == c, j // C, u))
        return j, k

    def collect(u, s, direct, extra=True):
        j, k = z_index(u, s)
        crossed = (r // 2 < j // 2) & (r % 2 != j % 2)
        landed = (r < j) & (crossed if direct else jnp.logical_not(crossed))
        if u >= U // 2:
            landed = landed & (j % C != c)
        landed = landed & extra

        for h in range(PARTS):
            block = xz.at[s, u, part(h)]

            @pl.when(landed)
            def _(block=block, h=h):
                arrive(block, xz_sem.at[s, u, h])

            if direct:
                send(landed, block, block, xz_sem.at[s, u, h], (r + 1 - 2 * (r % 2), c))

    def right(u, s):
        m = c + C * u

        def apply(a, dims):
            out[:, slot(u)] -= mm(own[s, 0], a, dims) + mm(own[s, 1], a, dims)

        def moved():
            if s > 0:
                arrive(atb.at[s, u], at_sem.at[s, u])

        if u >= U // 2:
            moved()
            apply(atb[s, u], NN)
            return
        plain = (m == r + 1) & (r != H - 1) if s > 0 else m < r

        @pl.when(m == r)
        def _():
            apply(upper[:, slot(u)] if s == 0 else an[u], NT)

        @pl.when((m != r) & plain)
        def _():
            moved()
            apply(atb[s, u], NT)

        @pl.when((m != r) & jnp.logical_not(plain))
        def _():
            moved()
            apply(atb[s, u], NN)

    def left(u, s):
        j, k = z_index(u, s)
        a = an[u] if s > 0 else upper[:, slot(u)]
        zh, zl = halves(decoded(s, k))

        def apply(dims):
            out[:, slot(u)] -= mm(a, zh, dims) + mm(a, zl, dims)

        low, high = C * u, C * u + C - 1
        if 2 * low >= d[s]:
            apply(NN)
        elif 2 * high < d[s]:
            apply(NT)
        else:
            m = c + C * u
            straight = d[s] - m <= m
            pl.when(straight)(lambda: apply(NN))
            pl.when(jnp.logical_not(straight))(lambda: apply(NT))

    def on_targets(s, fns, but=None):
        for u in range(U):
            live = target(r, c + C * u, s)
            if but is not None:
                live = live & jnp.logical_not(but(u))

            @pl.when(live)
            def _(u=u):
                for fn in fns:
                    fn(u, s)

    hand_right = pltpu.make_async_remote_copy(
        src_ref=ops.at[1], dst_ref=ops.at[1], send_sem=send_sem.at[0], recv_sem=ops_sem.at[1],
        device_id=(jnp.maximum(r - 1, 0), c), device_id_type=MESH)
    sends.append(((c == o[0]) & (r % 2 == 1), hand_right))

    @pl.when(c == o[0])
    def _():
        with scope("solve0"):
            prepare(0)
            solve(0)

    with scope("give0"):
        give_row(0)
        send_upper(c == o[0])
        send_turned(c == o[0])

    @pl.when(first)
    def _():
        with scope("prep"):
            prepare(1)

    with scope("take0"):
        take_row(0)
        pl.when(wants(c, 0) | first)(lambda: split_own(0))

    with scope("pick0"):
        for u in range(U // 2 - 1, U):
            collect(u, 0, True, picked(u))
            collect(u, 0, False, picked(u))

            @pl.when(picked(u))
            def _(u=u):
                right(u, 0)
                left(u, 0)

    @pl.when(first)
    def _():
        with scope("solve1"):
            solve(1)

    with scope("give1"):
        give_row(1)
        send_upper(None, True)

    def use_lower(rows):
        with scope("hand"):
            for u in range(U):
                @pl.when(rows & needs(u) & jnp.logical_not(ahead & (top == u)))
                def _(u=u):
                    arrive(atb.at[0, u], at_sem.at[0, u])

                hand_down(u, rows)
        with scope("right0"):
            on_targets(0, (right,), lambda u: picked(u) | jnp.logical_not(rows))

    with scope("direct0"):
        for u in range(U):
            collect(u, 0, True, jnp.logical_not(picked(u)))
    use_lower(r >= 2)
    with scope("collect0"):
        for u in range(U):
            collect(u, 0, False, jnp.logical_not(picked(u)))
    with scope("left0"):
        on_targets(0, (left,), picked)

    with scope("take1"):
        take_row(1)
        pl.when(wants(c, 1))(lambda: split_own(1))
    with scope("direct1"):
        for u in range(U):
            collect(u, 1, True)
    use_lower(r < 2)
    with scope("w_an"):
        for u in range(U):
            @pl.when(target(r, c + C * u, 1))
            def _(u=u):
                arrive(an.at[u], an_sem.at[u])
    with scope("right1"):
        on_targets(1, (right,))
    for u in range(U):
        with scope("collect1_%d" % u):
            collect(u, 1, False)

        @pl.when(target(r, c + C * u, 1))
        def _(u=u):
            with scope("left1_%d" % u):
                left(u, 1)

    def drain(some):
        for cond, copy in some:
            @pl.when(cond)
            def _(copy=copy):
                copy.wait_send()

    with scope("drain"):
        drain(sends)


def store(work, out, sem):
    lanes = work.shape[1] // out.shape[1]
    for j in range(out.shape[1]):
        pltpu.make_async_copy(work.at[:, pl.ds(j * lanes, lanes)], out.at[:, j, 0, :], sem.at[0]).start()
    pltpu.make_async_copy(work, work, sem.at[0]).wait()


def on_device(state, coupling, coupling_t, factor, cofactor, rates):
    R = lax.axis_size("row")
    C = lax.axis_size("col")
    U = 2 * R // C
    BS = state.shape[0]
    SR = factor.shape[2]
    flat = U * BS
    lanes = 128
    vmem = pl.BlockSpec(memory_space=pltpu.VMEM)
    hbm = pl.BlockSpec(memory_space=pltpu.HBM)
    dma = pltpu.SemaphoreType.DMA
    work = pl.pallas_call(
        functools.partial(kernel, R, C, U, BS, SR),
        out_shape=pltpu.VMEM((BS, flat), F32),
        in_specs=[hbm] * 6,
        out_specs=vmem,
        scratch_shapes=[
            pltpu.VMEM((BS, flat), BF16),
            pltpu.VMEM((2, BS, flat), BF16),
            pltpu.VMEM((U, BS, BS), BF16),
            pltpu.VMEM((2, U, SR, BS), F32),
            pltpu.VMEM((U, BS), F32),
            pltpu.VMEM((U, 2 * SR, BS), BF16),
            pltpu.VMEM((2, R, 2 * SR, BS), BF16),
            pltpu.VMEM((4, 2, BS, BS), BF16),
            pltpu.VMEM((U, BS), F32),
            pltpu.VMEM((STEPS, U + 1, PAD + BS, BS), BF16),
            pltpu.VMEM((STEPS, 2, BS, BS), BF16),
            pltpu.VMEM((STEPS, U, BS, BS), BF16),
            pltpu.VMEM((U, BS, BS), BF16),
            dma((5,)),
            dma((2,)),
            dma((1,)),
            dma((STEPS, U + 1, PARTS)),
            dma((STEPS, U)),
            dma((U,)),
            dma((1,)),
        ],
        compiler_params=pltpu.CompilerParams(
            collective_id=0, has_side_effects=True, vmem_limit_bytes=VMEM_LIMIT),
    )(
        state.reshape(BS, flat // lanes, 1, lanes),
        coupling.reshape(BS, flat),
        coupling_t.reshape(coupling_t.shape[0], BS, flat),
        factor.reshape(U, SR, BS),
        cofactor.reshape(U, SR, BS),
        rates,
    )
    out = pl.pallas_call(
        store,
        out_shape=jax.ShapeDtypeStruct((BS, flat // lanes, 1, lanes), F32),
        in_specs=[vmem],
        out_specs=hbm,
        scratch_shapes=[dma((1,))],
        compiler_params=pltpu.CompilerParams(vmem_limit_bytes=2 * 1024 * 1024),
    )(work)
    return out.reshape(BS, 1, flat)


VMEM_LIMIT = 61 * 1024 * 1024


def solution(mesh):
    return jax.shard_map(
        on_device,
        mesh=mesh,
        in_specs=(
            P("row", "col", None),
            P("row", "col", None),
            P(None, "row", "col", None),
            P(None, "col", "row", None),
            P(None, "col", "row", None),
            P(None, "col", None),
        ),
        out_specs=P("row", "col", None),
        check_vma=False,
    )
```

```python
import functools

import jax
import jax.numpy as jnp
from jax import lax
from jax.experimental import pallas as pl
from jax.experimental.pallas import tpu as pltpu
from jax.sharding import PartitionSpec as P

STEPS = 2
PARTS = 2
PAD = 16
SAME = 2
HOME = False
OP_MAX = 1.3
MESH = pl.DeviceIdType.MESH
F32 = jnp.float32
BF16 = jnp.bfloat16
NN = (((1,), (0,)), ((), ()))
NT = (((1,), (1,)), ((), ()))
scope = jax.named_scope


def halves(x):
    hi = x.astype(BF16)
    return hi, (x - hi.astype(F32)).astype(BF16)


def mm(a, b, dims):
    return lax.dot_general(a, b, dims, preferred_element_type=F32)


def dot3(a, b, dims):
    return mm(a[0], b[0], dims) + (mm(a[0], b[1], dims) + mm(a[1], b[0], dims))


def encode(x, inverse):
    v = jnp.exp2(jnp.sqrt(jnp.abs(x) * inverse) * 250.0 - 125.0)
    return jnp.where(x < 0, -v, v).astype(BF16)


def decode(v, scale):
    v = v.astype(F32)
    y = jnp.log2(jnp.abs(v)) * (1.0 / 250.0) + 0.5
    x = y * y * scale
    return jnp.where(v < 0, -x, x)


def kernel(R, C, U, BS, SR, state, upper_in, lower_in, factor, cofactor, rates_in, out,
           upper, lower, turned, raw, rates, enc, ops, mats, ebuf, xz, own, atb, an,
           load_sem, ops_sem, e_sem, xz_sem, at_sem, an_sem, send_sem):
    H = R // 2
    r = lax.axis_index("row")
    c = lax.axis_index("col")
    d = [2 * R - 1 - s for s in range(STEPS)]

    def owner(row, s):
        return (d[s] - row) % C

    o = [owner(r, s) for s in range(STEPS)]
    sends = []
    me = r * C + c

    barrier = pltpu.get_barrier_semaphore()

    pltpu.make_async_copy(cofactor, raw.at[0], load_sem.at[0]).start()
    pltpu.make_async_copy(factor, raw.at[1], load_sem.at[0]).start()

    @pl.loop(1, R * C)
    def _(k):
        peer = (me + k) % (R * C)
        pl.semaphore_signal(barrier, inc=1, device_id=(peer // C, peer % C), device_id_type=MESH)

    pltpu.make_async_copy(rates_in.at[:, 0, :], rates, load_sem.at[1]).start()
    pltpu.make_async_copy(lower_in, lower, load_sem.at[2]).start()
    lanes = out.shape[1] // state.shape[1]
    for j in range(state.shape[1]):
        pltpu.make_async_copy(state.at[:, j, 0, :], out.at[:, pl.ds(j * lanes, lanes)], load_sem.at[3]).start()
    pltpu.make_async_copy(upper_in, upper, load_sem.at[4]).start()

    def arrive(ref, sem):
        pltpu.make_async_copy(ref, ref, sem).wait()

    def send(cond, src, dst, sem, dev):
        copy = pltpu.make_async_remote_copy(
            src_ref=src, dst_ref=dst, send_sem=send_sem.at[0], recv_sem=sem,
            device_id=dev, device_id_type=MESH)
        sends.append((cond, copy))

        @pl.when(cond)
        def _():
            copy.start()

    def send_or_local(cond, src, dst, sem, dev):
        mine = (dev[0] == r) & (dev[1] == c)
        send(cond & jnp.logical_not(mine), src, dst, sem, dev)

        @pl.when(cond & mine)
        def _():
            pltpu.make_async_copy(src, dst, sem).start()

    def slot(u):
        if isinstance(u, int):
            return pl.ds(u * BS, BS)
        return pl.ds(pl.multiple_of(u * BS, BS), BS)

    def target(row, m, s):
        return (row <= m) & (row + m < d[s])

    with scope("encode"):
        arrive(raw, load_sem.at[0])
        for u in range(U):
            both = jnp.concatenate([raw[0, u], raw[1, u]], axis=0)
            enc[u] = encode(both, 1.0 / OP_MAX)
        arrive(rates, load_sem.at[1])

    with scope("barrier"):
        pl.semaphore_wait(barrier, R * C - 1)

    def send_left(s):
        for u in range(U // 2):
            m = c + C * u
            send_or_local(m < R, enc.at[u], ops.at[0, r], ops_sem.at[0], (m, owner(m, s)))

    def send_right(s):
        for u in range(U // 2 - s, U):
            to = d[s] - (c + C * u)
            live = (to >= 0) & (to < R)
            if s > 0:
                live = live & (to % 2 == 1)
            send_or_local(live, enc.at[u], ops.at[1, r], ops_sem.at[1], (to, c))

    def send_lower(first):
        to = (r + H) % R
        top = (d[0] - 1 - to - c) // C
        for u in range(U - 1, -1, -1):
            m = c + C * u
            turn = u == top if first else u != top
            send(target(to, m, 0) & (m != to) & turn, lower.at[0, :, slot(u)], atb.at[0, u], at_sem.at[0, u], (to, c))

    def send_middle():
        for u in range(U):
            m = c + C * u
            send((r == 0) & (m >= H) & target(H - 1, m, 1), lower.at[0, :, slot(u)], atb.at[1, u],
                 at_sem.at[1, u], (H - 1, c))

    q1 = (d[1] - r) // C
    first = c == o[1]
    top = (d[0] - 1 - r - c) // C
    ahead = c != o[0]

    def needs(u):
        m = c + C * u
        return target(r, m, 0) & (m != r)

    def picked(u):
        return first & (q1 == u)

    def crossing(i, m):
        beside = ((m + 1 + H) % R) // 2 == i // 2
        same = (m - i) % C == 0
        return (m % C == C - 1) | (same & beside if SAME == 1 else same if SAME else False)

    def send_turned(cond):
        for t in range(2):
            m = (r + H) % R + R * t - 1
            for u in range(U // 2):
                i = c + C * u
                live = cond & (m >= 0) & target(i, m, 1) & crossing(i, m)
                to_u = jnp.clip(m // C, 0, U - 1)
                mine = (i == r) & (m % C == c)
                k = t * (U // 2) + u

                @pl.when(live)
                def _(t=t, u=u, k=k):
                    turned[k] = jnp.transpose(lower[t, :, slot(u)])

                send(live & jnp.logical_not(mine), turned.at[k], an.at[to_u], an_sem.at[to_u], (i, m % C))

                @pl.when(live & mine)
                def _(k=k, to_u=to_u):
                    pltpu.make_async_copy(turned.at[k], an.at[to_u], an_sem.at[to_u]).start()

    def send_upper(cond, held=None):
        late = first & (r % 2 == 0)
        for u in range(U):
            m = c + C * u - 1
            to = (c + C - 1) % C
            to_u = jnp.maximum(jnp.where(c >= 1, u, u - 1), 0)
            if u >= U // 2:
                now = late if held else cond & jnp.logical_not(late)
            elif held:
                continue
            else:
                now = cond
            send(now & jnp.logical_not(crossing(r, m)) & (m >= 0) & target(r, m, 1), upper.at[:, slot(u)], an.at[to_u],
                 an_sem.at[to_u], (r, to))

    def hand_down(u):
        m = c + C * u
        live = (r >= 1) & (r != H) & (m >= r) & target(r - 1, m, 1)
        to = (jnp.maximum(r - 1, 0), c)
        if u < U // 2:
            send(live & (m == r), upper.at[:, slot(u)], atb.at[1, u], at_sem.at[1, u], to)
        send(live & (m != r), atb.at[0, u], atb.at[1, u], at_sem.at[1, u], to)

    with scope("sends0"):
        send_left(0)
        send_right(0)
        for s in range(STEPS):
            send_or_local(c == r % C, rates, ebuf, e_sem.at[0], (r, o[s]))
        send_left(1)
        arrive(lower, load_sem.at[2])
        send_lower(True)
        send_right(1)
        send_lower(False)
        send_middle()
        arrive(upper, load_sem.at[4])
        arrive(out, load_sem.at[3])
        send_upper(c != o[0])

    with scope("gate"):
        @pl.when(ahead & needs(top))
        def _():
            arrive(atb.at[0, top], at_sem.at[0, top])

        send_turned(c != o[0])

    half = BS // PARTS

    def part(h):
        if h == 0:
            return pl.ds(0, PAD + half)
        return pl.ds(PAD + h * half, half)

    def spread(s, h, who):
        home = r % C
        own_col = home == c
        k = jnp.where(own_col, r // C, (d[s] - r) // C)
        has = (c == o[s]) & who if s > 0 and HOME else (own_col | (c == o[s])) & who

        def give(cond, to):
            if s > 0 and HOME:
                send(cond & has & (home != c), xz.at[s, U, part(h)], xz.at[s, r // C, part(h)],
                     xz_sem.at[s, r // C, h], (to, home))
            send(cond & has, xz.at[s, U, part(h)], xz.at[s, k, part(h)], xz_sem.at[s, k, h], (to, c))

        give(r % 2 == 1, jnp.maximum(r - 1, 0))
        for back in range(R // 2 - 1, 0, -1) if s > 0 else range(1, R // 2):
            pair = r // 2 - back
            give(pair >= 0, jnp.maximum(2 * pair + 1 - r % 2, 0))

    def wants(col, s):
        return (col - r) % C < d[s] - 2 * r

    def give_row(s):
        at = c == o[s]
        home = r % C
        goal = (o[s] + C - 1) % C
        def give(cond, to):
            for h in range(PARTS):
                block = xz.at[s, U, part(h)]
                send(at & cond, block, block, xz_sem.at[s, U, h], (r, jnp.clip(to, 0, C - 1)))

        if s == 0:
            give(True, goal)
        for h in range(PARTS):
            spread(s, h, at)
        give((home != c) & (home != goal) if s == 0 else home != c, home)
        for far_by in range(C - 1, 0, -1):
            for to in (c - far_by, c + far_by):
                live = (to >= 0) & (to < C) & (to != home) & wants(to, s)
                if s == 0:
                    live = live & (to != goal)
                give(live, to)

    def take_row(s):
        other = (c != o[s]) & (wants(c, s) | (c == r % C))
        if s == 0:
            other = other | first
        for h in range(PARTS):
            block = xz.at[s, U, part(h)]
            sem = xz_sem.at[s, U, h]

            @pl.when(other)
            def _(block=block, sem=sem):
                arrive(block, sem)

            if s == 0 or not HOME:
                spread(s, h, other)

    def decoded(s, k):
        return decode(xz[s, k, PAD:], xz[s, k, 0:1, :].astype(F32))

    def split_own(s):
        xh, xl = halves(decoded(s, U))
        own[s, 0] = xh
        own[s, 1] = xl

    def prepare(s):
        with scope("w_e"):
            arrive(ebuf, e_sem.at[0])
        group = max(1, 16 // SR)
        for side in range(2):
            with scope("w_op%d" % side):
                arrive(ops.at[side], ops_sem.at[side])
            if s == 0 and side == 1:
                pl.when(r % 2 == 1)(hand_right.start)
            for k in range(0, R, group):
                both = [decode(ops[side, k + i], OP_MAX) for i in range(group)]
                for which in range(2):
                    rows = [b[which * SR:(which + 1) * SR] for b in both]
                    hi, lo = halves(rows[0] if group == 1 else jnp.concatenate(rows, axis=0))
                    mats[2 * side + which, 0, k * SR:(k + group) * SR] = hi
                    mats[2 * side + which, 1, k * SR:(k + group) * SR] = lo

    def solve(s):
        q = (d[s] - r) // C
        left_e = jnp.transpose(jnp.broadcast_to(ebuf[pl.ds(r // C, 1), :], (BS, BS)))
        rate = left_e + rates[pl.ds(q, 1), :]
        mat = [(mats[k, 0], mats[k, 1]) for k in range(4)]
        mid = dot3(mat[0], halves(out[:, slot(q)]), NN)
        mid = dot3(halves(mid), mat[2], NT) / rate
        mid = dot3(mat[1], halves(mid), NN)
        x = -dot3(halves(mid), mat[3], NT)
        out[:, slot(q)] = x
        peak = jnp.max(jnp.abs(x), axis=0, keepdims=True) * 1.01 + 1e-30
        scale = peak.astype(BF16)
        xz[s, U, :PAD] = jnp.broadcast_to(scale, (PAD, BS))
        xz[s, U, PAD:] = encode(x, 1.0 / scale.astype(F32))

    def z_index(u, s):
        m = c + C * u
        j = jnp.where(d[s] - m <= m, d[s] - m, m)
        k = jnp.where(j == r, U, jnp.where(j % C == c, j // C, u))
        return j, k

    def collect(u, s, direct, extra=True):
        j, k = z_index(u, s)
        crossed = (r // 2 < j // 2) & (r % 2 != j % 2)
        landed = (r < j) & (crossed if direct else jnp.logical_not(crossed))
        if u >= U // 2:
            landed = landed & (j % C != c)
        landed = landed & extra

        for h in range(PARTS):
            block = xz.at[s, u, part(h)]

            @pl.when(landed)
            def _(block=block, h=h):
                arrive(block, xz_sem.at[s, u, h])

            if direct:
                send(landed, block, block, xz_sem.at[s, u, h], (r + 1 - 2 * (r % 2), c))

    def right(u, s):
        m = c + C * u

        def apply(a, dims):
            out[:, slot(u)] -= mm(own[s, 0], a, dims) + mm(own[s, 1], a, dims)

        def moved():
            if s > 0:
                arrive(atb.at[s, u], at_sem.at[s, u])

        if u >= U // 2:
            moved()
            apply(atb[s, u], NN)
            return
        plain = (m == r + 1) & (r != H - 1) if s > 0 else m < r

        @pl.when(m == r)
        def _():
            apply(upper[:, slot(u)] if s == 0 else an[u], NT)

        @pl.when((m != r) & plain)
        def _():
            moved()
            apply(atb[s, u], NT)

        @pl.when((m != r) & jnp.logical_not(plain))
        def _():
            moved()
            apply(atb[s, u], NN)

    def left(u, s):
        j, k = z_index(u, s)
        a = an[u] if s > 0 else upper[:, slot(u)]
        zh, zl = halves(decoded(s, k))

        def apply(dims):
            out[:, slot(u)] -= mm(a, zh, dims) + mm(a, zl, dims)

        low, high = C * u, C * u + C - 1
        if 2 * low >= d[s]:
            apply(NN)
        elif 2 * high < d[s]:
            apply(NT)
        else:
            m = c + C * u
            straight = d[s] - m <= m
            pl.when(straight)(lambda: apply(NN))
            pl.when(jnp.logical_not(straight))(lambda: apply(NT))

    hand_right = pltpu.make_async_remote_copy(
        src_ref=ops.at[1], dst_ref=ops.at[1], send_sem=send_sem.at[0], recv_sem=ops_sem.at[1],
        device_id=(jnp.maximum(r - 1, 0), c), device_id_type=MESH)
    sends.append(((c == o[0]) & (r % 2 == 1), hand_right))

    @pl.when(c == o[0])
    def _():
        with scope("solve0"):
            prepare(0)
            solve(0)

    with scope("give0"):
        give_row(0)
        send_upper(c == o[0])
        send_turned(c == o[0])

    @pl.when(first)
    def _():
        with scope("prep"):
            prepare(1)

    with scope("take0"):
        take_row(0)
        pl.when(wants(c, 0) | first)(lambda: split_own(0))

    with scope("pick0"):
        for u in range(U // 2 - 1, U):
            collect(u, 0, True, picked(u))
            collect(u, 0, False, picked(u))

            @pl.when(picked(u))
            def _(u=u):
                right(u, 0)
                left(u, 0)

    @pl.when(first)
    def _():
        with scope("solve1"):
            solve(1)

    with scope("give1"):
        give_row(1)
        send_upper(None, True)

    def at_hand(u, s):
        j, k = z_index(u, s)
        return (j == r) | ((r // 2 < j // 2) & (r % 2 != j % 2))

    def use_right(s, u):
        pl.when(target(r, c + C * u, s) & jnp.logical_not(picked(u) if s == 0 else False))(lambda: right(u, s))

    def use_left(s, u, here):
        live = target(r, c + C * u, s) & (at_hand(u, s) if here else jnp.logical_not(at_hand(u, s)))
        if s == 0:
            live = live & jnp.logical_not(picked(u))

        @pl.when(live)
        def _():
            if s > 0:
                arrive(an.at[u], an_sem.at[u])
            left(u, s)

    with scope("direct0"):
        for u in range(U):
            collect(u, 0, True, jnp.logical_not(picked(u)))
    with scope("leftA0"):
        for u in range(U):
            use_left(0, u, True)
    with scope("hand"):
        for u in range(U - 1, -1, -1):
            @pl.when(needs(u) & jnp.logical_not(ahead & (top == u)))
            def _(u=u):
                arrive(atb.at[0, u], at_sem.at[0, u])

            hand_down(u)
    with scope("right0"):
        for u in range(U):
            use_right(0, u)
    with scope("leftB0"):
        for u in range(U - 1, -1, -1):
            collect(u, 0, False, jnp.logical_not(picked(u)))
            use_left(0, u, False)

    with scope("take1"):
        take_row(1)
        pl.when(wants(c, 1))(lambda: split_own(1))
    with scope("direct1"):
        for u in range(U):
            collect(u, 1, True)
    with scope("leftA1"):
        for u in range(U):
            use_left(1, u, True)
    with scope("right1"):
        for u in range(U):
            use_right(1, u)
    with scope("drain"):
        for cond, copy in sends:
            @pl.when(cond)
            def _(copy=copy):
                copy.wait_send()
    for u in range(U):
        with scope("leftB1_%d" % u):
            collect(u, 1, False)
            use_left(1, u, False)


def store(work, out, sem):
    lanes = work.shape[1] // out.shape[1]
    for j in range(out.shape[1]):
        pltpu.make_async_copy(work.at[:, pl.ds(j * lanes, lanes)], out.at[:, j, 0, :], sem.at[0]).start()
    pltpu.make_async_copy(work, work, sem.at[0]).wait()


def on_device(state, coupling, coupling_t, factor, cofactor, rates):
    R = lax.axis_size("row")
    C = lax.axis_size("col")
    U = 2 * R // C
    BS = state.shape[0]
    SR = factor.shape[2]
    flat = U * BS
    lanes = 128
    vmem = pl.BlockSpec(memory_space=pltpu.VMEM)
    hbm = pl.BlockSpec(memory_space=pltpu.HBM)
    dma = pltpu.SemaphoreType.DMA
    work = pl.pallas_call(
        functools.partial(kernel, R, C, U, BS, SR),
        out_shape=pltpu.VMEM((BS, flat), F32),
        in_specs=[hbm] * 6,
        out_specs=vmem,
        scratch_shapes=[
            pltpu.VMEM((BS, flat), BF16),
            pltpu.VMEM((2, BS, flat), BF16),
            pltpu.VMEM((U, BS, BS), BF16),
            pltpu.VMEM((2, U, SR, BS), F32),
            pltpu.VMEM((U, BS), F32),
            pltpu.VMEM((U, 2 * SR, BS), BF16),
            pltpu.VMEM((2, R, 2 * SR, BS), BF16),
            pltpu.VMEM((4, 2, BS, BS), BF16),
            pltpu.VMEM((U, BS), F32),
            pltpu.VMEM((STEPS, U + 1, PAD + BS, BS), BF16),
            pltpu.VMEM((STEPS, 2, BS, BS), BF16),
            pltpu.VMEM((STEPS, U, BS, BS), BF16),
            pltpu.VMEM((U, BS, BS), BF16),
            dma((5,)),
            dma((2,)),
            dma((1,)),
            dma((STEPS, U + 1, PARTS)),
            dma((STEPS, U)),
            dma((U,)),
            dma((1,)),
        ],
        compiler_params=pltpu.CompilerParams(
            collective_id=0, has_side_effects=True, vmem_limit_bytes=VMEM_LIMIT),
    )(
        state.reshape(BS, flat // lanes, 1, lanes),
        coupling.reshape(BS, flat),
        coupling_t.reshape(coupling_t.shape[0], BS, flat),
        factor.reshape(U, SR, BS),
        cofactor.reshape(U, SR, BS),
        rates,
    )
    out = pl.pallas_call(
        store,
        out_shape=jax.ShapeDtypeStruct((BS, flat // lanes, 1, lanes), F32),
        in_specs=[vmem],
        out_specs=hbm,
        scratch_shapes=[dma((1,))],
        compiler_params=pltpu.CompilerParams(vmem_limit_bytes=2 * 1024 * 1024),
    )(work)
    return out.reshape(BS, 1, flat)


VMEM_LIMIT = 61 * 1024 * 1024


def solution(mesh):
    return jax.shard_map(
        on_device,
        mesh=mesh,
        in_specs=(
            P("row", "col", None),
            P("row", "col", None),
            P(None, "row", "col", None),
            P(None, "col", "row", None),
            P(None, "col", "row", None),
            P(None, "col", None),
        ),
        out_specs=P("row", "col", None),
        check_vma=False,
    )
```

```python
import functools

import jax
import jax.numpy as jnp
from jax import lax
from jax.experimental import pallas as pl
from jax.experimental.pallas import tpu as pltpu
from jax.sharding import PartitionSpec as P

STEPS = 2
PARTS = 2
PAD = 16
SAME = 2
HOME = False
RELAY = (False, False)
FORWARD = True
OP_MAX = 1.3
MESH = pl.DeviceIdType.MESH
F32 = jnp.float32
BF16 = jnp.bfloat16
NN = (((1,), (0,)), ((), ()))
NT = (((1,), (1,)), ((), ()))
scope = jax.named_scope


def halves(x):
    hi = x.astype(BF16)
    return hi, (x - hi.astype(F32)).astype(BF16)


def mm(a, b, dims):
    return lax.dot_general(a, b, dims, preferred_element_type=F32)


def dot3(a, b, dims):
    return mm(a[0], b[0], dims) + (mm(a[0], b[1], dims) + mm(a[1], b[0], dims))


def encode(x, inverse):
    v = jnp.exp2(jnp.sqrt(jnp.abs(x) * inverse) * 250.0 - 125.0)
    return jnp.where(x < 0, -v, v).astype(BF16)


def decode(v, scale):
    v = v.astype(F32)
    y = jnp.log2(jnp.abs(v)) * (1.0 / 250.0) + 0.5
    x = y * y * scale
    return jnp.where(v < 0, -x, x)


def kernel(R, C, U, BS, SR, state, upper_in, lower_in, factor, cofactor, rates_in, out,
           upper, lower, turned, raw, rates, enc, ops, mats, ebuf, xz, own, atb, an,
           load_sem, ops_sem, e_sem, xz_sem, at_sem, an_sem, send_sem):
    H = R // 2
    r = lax.axis_index("row")
    c = lax.axis_index("col")
    d = [2 * R - 1 - s for s in range(STEPS)]

    def owner(row, s):
        return (d[s] - row) % C

    o = [owner(r, s) for s in range(STEPS)]
    sends = []
    me = r * C + c

    barrier = pltpu.get_barrier_semaphore()

    pltpu.make_async_copy(cofactor, raw.at[0], load_sem.at[0]).start()
    pltpu.make_async_copy(factor, raw.at[1], load_sem.at[0]).start()

    @pl.loop(1, R * C)
    def _(k):
        peer = (me + k) % (R * C)
        pl.semaphore_signal(barrier, inc=1, device_id=(peer // C, peer % C), device_id_type=MESH)

    pltpu.make_async_copy(rates_in.at[:, 0, :], rates, load_sem.at[1]).start()
    pltpu.make_async_copy(lower_in, lower, load_sem.at[2]).start()
    lanes = out.shape[1] // state.shape[1]
    for j in range(state.shape[1]):
        pltpu.make_async_copy(state.at[:, j, 0, :], out.at[:, pl.ds(j * lanes, lanes)], load_sem.at[3]).start()
    pltpu.make_async_copy(upper_in, upper, load_sem.at[4]).start()

    def arrive(ref, sem):
        pltpu.make_async_copy(ref, ref, sem).wait()

    def send(cond, src, dst, sem, dev):
        copy = pltpu.make_async_remote_copy(
            src_ref=src, dst_ref=dst, send_sem=send_sem.at[0], recv_sem=sem,
            device_id=dev, device_id_type=MESH)
        sends.append((cond, copy, (src.shape, str(src.dtype))))

        @pl.when(cond)
        def _():
            copy.start()

    def send_or_local(cond, src, dst, sem, dev):
        mine = (dev[0] == r) & (dev[1] == c)
        send(cond & jnp.logical_not(mine), src, dst, sem, dev)

        @pl.when(cond & mine)
        def _():
            pltpu.make_async_copy(src, dst, sem).start()

    def slot(u):
        if isinstance(u, int):
            return pl.ds(u * BS, BS)
        return pl.ds(pl.multiple_of(u * BS, BS), BS)

    def target(row, m, s):
        return (row <= m) & (row + m < d[s])

    with scope("encode"):
        arrive(raw, load_sem.at[0])
        for u in range(U):
            both = jnp.concatenate([raw[0, u], raw[1, u]], axis=0)
            enc[u] = encode(both, 1.0 / OP_MAX)
        arrive(rates, load_sem.at[1])

    with scope("barrier"):
        pl.semaphore_wait(barrier, R * C - 1)

    def send_left(s):
        for u in range(U // 2):
            m = c + C * u
            send_or_local(m < R, enc.at[u], ops.at[0, r], ops_sem.at[0], (m, owner(m, s)))

    def send_right(s):
        for u in range(U // 2 - s, U):
            to = d[s] - (c + C * u)
            live = (to >= 0) & (to < R)
            if s > 0:
                live = live & (to % 4 == 3 if FORWARD else to % 2 == 1)
            send_or_local(live, enc.at[u], ops.at[1, r], ops_sem.at[1], (to, c))

    def send_lower(first):
        to = (r + H) % R
        top = (d[0] - 1 - to - c) // C
        for u in range(U - 1, -1, -1):
            m = c + C * u
            turn = u == top if first else u != top
            send(target(to, m, 0) & (m != to) & turn, lower.at[0, :, slot(u)], atb.at[0, u], at_sem.at[0, u], (to, c))

    def send_middle():
        for u in range(U):
            m = c + C * u
            send((r == 0) & (m >= H) & target(H - 1, m, 1), lower.at[0, :, slot(u)], atb.at[1, u],
                 at_sem.at[1, u], (H - 1, c))

    q1 = (d[1] - r) // C
    first = c == o[1]
    top = (d[0] - 1 - r - c) // C
    ahead = c != o[0]

    def needs(u):
        m = c + C * u
        return target(r, m, 0) & (m != r)

    def picked(u):
        return first & (q1 == u)

    def crossing(i, m):
        beside = ((m + 1 + H) % R) // 2 == i // 2
        same = (m - i) % C == 0
        return (m % C == C - 1) | (same & beside if SAME == 1 else same if SAME else False)

    def send_turned(cond):
        for t in range(2):
            m = (r + H) % R + R * t - 1
            for u in range(U // 2):
                i = c + C * u
                live = cond & (m >= 0) & target(i, m, 1) & crossing(i, m)
                to_u = jnp.clip(m // C, 0, U - 1)
                mine = (i == r) & (m % C == c)
                k = t * (U // 2) + u

                @pl.when(live)
                def _(t=t, u=u, k=k):
                    turned[k] = jnp.transpose(lower[t, :, slot(u)])

                send(live & jnp.logical_not(mine), turned.at[k], an.at[to_u], an_sem.at[to_u], (i, m % C))

                @pl.when(live & mine)
                def _(k=k, to_u=to_u):
                    pltpu.make_async_copy(turned.at[k], an.at[to_u], an_sem.at[to_u]).start()

    def send_upper(cond, held=None):
        late = first & (r % 2 == 0)
        for u in range(U):
            m = c + C * u - 1
            to = (c + C - 1) % C
            to_u = jnp.maximum(jnp.where(c >= 1, u, u - 1), 0)
            if u >= U // 2:
                now = late if held else cond & jnp.logical_not(late)
            elif held:
                continue
            else:
                now = cond
            send(now & jnp.logical_not(crossing(r, m)) & (m >= 0) & target(r, m, 1), upper.at[:, slot(u)], an.at[to_u],
                 an_sem.at[to_u], (r, to))

    def hand_down(u):
        m = c + C * u
        live = (r >= 1) & (r != H) & (m >= r) & target(r - 1, m, 1)
        to = (jnp.maximum(r - 1, 0), c)
        send(live, atb.at[0, u], atb.at[1, u], at_sem.at[1, u], to)

    with scope("sends0"):
        send_left(0)
        send_right(0)
        for s in range(STEPS):
            send_or_local(c == r % C, rates, ebuf, e_sem.at[0], (r, o[s]))
        send_left(1)
        arrive(lower, load_sem.at[2])
        send_lower(True)
        send_right(1)
        send_lower(False)
        send_middle()
        arrive(upper, load_sem.at[4])
        arrive(out, load_sem.at[3])
        send_upper(c != o[0])

    with scope("gate"):
        @pl.when(ahead & needs(top))
        def _():
            arrive(atb.at[0, top], at_sem.at[0, top])

        send_turned(c != o[0])
        for u in range(U // 2):
            @pl.when(target(r, c + C * u, 0) & (c + C * u == r))
            def _(u=u):
                atb[0, u] = jnp.transpose(upper[:, slot(u)])

    half = BS // PARTS

    def part(h):
        if h == 0:
            return pl.ds(0, PAD + half)
        return pl.ds(PAD + h * half, half)

    def spread(s, h, who):
        home = r % C
        own_col = home == c
        k = jnp.where(own_col, r // C, (d[s] - r) // C)
        has = (c == o[s]) & who if s > 0 and HOME else (own_col | (c == o[s])) & who

        def give(cond, to):
            if s > 0 and HOME:
                send(cond & has & (home != c), xz.at[s, U, part(h)], xz.at[s, r // C, part(h)],
                     xz_sem.at[s, r // C, h], (to, home))
            send(cond & has, xz.at[s, U, part(h)], xz.at[s, k, part(h)], xz_sem.at[s, k, h], (to, c))

        give(r % 2 == 1, jnp.maximum(r - 1, 0))
        for back in range(R // 2 - 1, 0, -1) if s > 0 else range(1, R // 2):
            if back == 3 and RELAY[s]:
                continue
            pair = r // 2 - back
            give(pair >= 0, jnp.maximum(2 * pair + 1 - r % 2, 0))

    def wants(col, s):
        return (col - r) % C < d[s] - 2 * r

    def give_row(s):
        at = c == o[s]
        home = r % C
        goal = (o[s] + C - 1) % C
        def give(cond, to):
            for h in range(PARTS):
                block = xz.at[s, U, part(h)]
                send(at & cond, block, block, xz_sem.at[s, U, h], (r, jnp.clip(to, 0, C - 1)))

        if s == 0:
            give(True, goal)
        for h in range(PARTS):
            spread(s, h, at)
        give((home != c) & (home != goal) if s == 0 else home != c, home)
        for far_by in range(C - 1, 0, -1):
            for to in (c - far_by, c + far_by):
                live = (to >= 0) & (to < C) & (to != home) & wants(to, s)
                if s == 0:
                    live = live & (to != goal)
                give(live, to)

    def take_row(s):
        other = (c != o[s]) & (wants(c, s) | (c == r % C))
        if s == 0:
            other = other | first
        for h in range(PARTS):
            block = xz.at[s, U, part(h)]
            sem = xz_sem.at[s, U, h]

            @pl.when(other)
            def _(block=block, sem=sem):
                arrive(block, sem)

            if s == 0 or not HOME:
                spread(s, h, other)

    def decoded(s, k):
        return decode(xz[s, k, PAD:], xz[s, k, 0:1, :].astype(F32))

    def split_own(s):
        xh, xl = halves(decoded(s, U))
        own[s, 0] = xh
        own[s, 1] = xl

    def prepare(s):
        with scope("w_e"):
            arrive(ebuf, e_sem.at[0])
        group = max(1, 16 // SR)
        for side in range(2):
            with scope("w_op%d" % side):
                arrive(ops.at[side], ops_sem.at[side])
            if s == 0 and side == 1:
                pl.when(hands)(hand_right.start)
            for k in range(0, R, group):
                both = [decode(ops[side, k + i], OP_MAX) for i in range(group)]
                for which in range(2):
                    rows = [b[which * SR:(which + 1) * SR] for b in both]
                    hi, lo = halves(rows[0] if group == 1 else jnp.concatenate(rows, axis=0))
                    mats[2 * side + which, 0, k * SR:(k + group) * SR] = hi
                    mats[2 * side + which, 1, k * SR:(k + group) * SR] = lo

    def solve(s):
        q = (d[s] - r) // C
        left_e = jnp.transpose(jnp.broadcast_to(ebuf[pl.ds(r // C, 1), :], (BS, BS)))
        rate = left_e + rates[pl.ds(q, 1), :]
        mat = [(mats[k, 0], mats[k, 1]) for k in range(4)]
        mid = dot3(mat[0], halves(out[:, slot(q)]), NN)
        mid = dot3(halves(mid), mat[2], NT) / rate
        mid = dot3(mat[1], halves(mid), NN)
        x = -dot3(halves(mid), mat[3], NT)
        out[:, slot(q)] = x
        peak = jnp.max(jnp.abs(x), axis=0, keepdims=True) * 1.01 + 1e-30
        scale = peak.astype(BF16)
        xz[s, U, :PAD] = jnp.broadcast_to(scale, (PAD, BS))
        xz[s, U, PAD:] = encode(x, 1.0 / scale.astype(F32))

    def z_index(u, s):
        m = c + C * u
        j = jnp.where(d[s] - m <= m, d[s] - m, m)
        k = jnp.where(j == r, U, jnp.where(j % C == c, j // C, u))
        return j, k

    def collect(u, s, direct, extra=True):
        j, k = z_index(u, s)
        crossed = (r // 2 < j // 2) & (r % 2 != j % 2)
        landed = (r < j) & (crossed if direct else jnp.logical_not(crossed))
        if u >= U // 2:
            landed = landed & (j % C != c)
        landed = landed & extra

        for h in range(PARTS):
            block = xz.at[s, u, part(h)]

            @pl.when(landed)
            def _(block=block, h=h):
                arrive(block, xz_sem.at[s, u, h])

            if direct:
                send(landed, block, block, xz_sem.at[s, u, h], (r + 1 - 2 * (r % 2), c))
                if RELAY[s]:
                    on = landed & (r // 2 >= 1) & (j // 2 - r // 2 == 2)
                    send(on, block, block, xz_sem.at[s, u, h], (jnp.maximum(r - 2, 0), c))

    def update(u, s):
        m = c + C * u
        j, k = z_index(u, s)

        if s > 0:
            @pl.when(m != r)
            def _():
                arrive(atb.at[s, u], at_sem.at[s, u])

        def apply(dims):
            a = an[u] if s > 0 else upper[:, slot(u)]
            zh, zl = halves(decoded(s, k))
            row = mm(own[s, 0], atb[s, u], NN) + mm(own[s, 1], atb[s, u], NN)
            out[:, slot(u)] -= row + (mm(a, zh, dims) + mm(a, zl, dims))

        low, high = C * u, C * u + C - 1
        if 2 * low >= d[s]:
            apply(NN)
        elif 2 * high < d[s]:
            apply(NT)
        else:
            straight = d[s] - m <= m
            pl.when(straight)(lambda: apply(NN))
            pl.when(jnp.logical_not(straight))(lambda: apply(NT))

    hand_right = pltpu.make_async_remote_copy(
        src_ref=ops.at[1], dst_ref=ops.at[1], send_sem=send_sem.at[0], recv_sem=ops_sem.at[1],
        device_id=(jnp.maximum(r - 1, 0), c), device_id_type=MESH)
    hands = r % 4 != 0 if FORWARD else r % 2 == 1
    sends.append(((c == o[0]) & hands, hand_right, ops.at[1].shape))

    @pl.when(c == o[0])
    def _():
        with scope("solve0"):
            prepare(0)
            solve(0)

    with scope("give0"):
        give_row(0)
        send_upper(c == o[0])
        send_turned(c == o[0])

    @pl.when(first)
    def _():
        with scope("prep"):
            prepare(1)

    with scope("take0"):
        take_row(0)
        pl.when(wants(c, 0) | first)(lambda: split_own(0))

    with scope("pick0"):
        for u in range(U // 2 - 1, U):
            collect(u, 0, True, picked(u))
            collect(u, 0, False, picked(u))

            @pl.when(picked(u))
            def _(u=u):
                update(u, 0)

    @pl.when(first)
    def _():
        with scope("solve1"):
            solve(1)

    with scope("give1"):
        give_row(1)
        send_upper(None, True)

    def at_hand(u, s):
        j, k = z_index(u, s)
        return (j == r) | ((r // 2 < j // 2) & (r % 2 != j % 2))

    def use(s, u, here, also=True):
        live = also & target(r, c + C * u, s) & (at_hand(u, s) if here else jnp.logical_not(at_hand(u, s)))
        if s == 0:
            live = live & jnp.logical_not(picked(u))
        pl.when(live)(lambda: update(u, s))

    with scope("direct0"):
        for u in range(U - 1, -1, -1):
            collect(u, 0, True, jnp.logical_not(picked(u)))
    with scope("hand"):
        for u in range(U - 1, -1, -1):
            @pl.when(needs(u) & jnp.logical_not(ahead & (top == u)))
            def _(u=u):
                arrive(atb.at[0, u], at_sem.at[0, u])

            hand_down(u)
    with scope("A0"):
        for u in range(U):
            use(0, u, True)
    with scope("B0"):
        for u in range(U - 1, -1, -1):
            collect(u, 0, False, jnp.logical_not(picked(u)))
            use(0, u, False)

    with scope("take1"):
        take_row(1)
        pl.when(wants(c, 1))(lambda: split_own(1))
    with scope("direct1"):
        for u in range(U - 1, -1, -1):
            collect(u, 1, True)
    with scope("w_an"):
        for u in range(U):
            m = c + C * u

            @pl.when(target(r, m, 1))
            def _(u=u):
                arrive(an.at[u], an_sem.at[u])

            if u < U // 2:
                @pl.when(target(r, m, 1) & (m == r))
                def _(u=u):
                    atb[1, u] = jnp.transpose(an[u])
    with scope("A1"):
        for u in range(U):
            use(1, u, True)
    with scope("drain"):
        sizes = {}
        for cond, copy, size in sends:
            sizes.setdefault(size, []).append((cond, copy))
        for group in sizes.values():
            count = sum(jnp.where(cond, 1, 0) for cond, _ in group)

            @pl.loop(0, count)
            def _(_, copy=group[0][1]):
                copy.wait_send()
    def twice(u):
        j, k = z_index(u, 1)
        return (u >= U // 2) & (j % C == c)

    for u in range(U - 1, -1, -1):
        with scope("B1_%d" % u):
            collect(u, 1, False)
            use(1, u, False, jnp.logical_not(twice(u)))
    for u in range(U // 2, U):
        with scope("C1_%d" % u):
            use(1, u, False, twice(u))


def store(work, out, sem):
    lanes = work.shape[1] // out.shape[1]
    for j in range(out.shape[1]):
        pltpu.make_async_copy(work.at[:, pl.ds(j * lanes, lanes)], out.at[:, j, 0, :], sem.at[0]).start()
    pltpu.make_async_copy(work, work, sem.at[0]).wait()


def on_device(state, coupling, coupling_t, factor, cofactor, rates):
    R = lax.axis_size("row")
    C = lax.axis_size("col")
    U = 2 * R // C
    BS = state.shape[0]
    SR = factor.shape[2]
    flat = U * BS
    lanes = 128
    vmem = pl.BlockSpec(memory_space=pltpu.VMEM)
    hbm = pl.BlockSpec(memory_space=pltpu.HBM)
    dma = pltpu.SemaphoreType.DMA
    work = pl.pallas_call(
        functools.partial(kernel, R, C, U, BS, SR),
        out_shape=pltpu.VMEM((BS, flat), F32),
        in_specs=[hbm] * 6,
        out_specs=vmem,
        scratch_shapes=[
            pltpu.VMEM((BS, flat), BF16),
            pltpu.VMEM((2, BS, flat), BF16),
            pltpu.VMEM((U, BS, BS), BF16),
            pltpu.VMEM((2, U, SR, BS), F32),
            pltpu.VMEM((U, BS), F32),
            pltpu.VMEM((U, 2 * SR, BS), BF16),
            pltpu.VMEM((2, R, 2 * SR, BS), BF16),
            pltpu.VMEM((4, 2, BS, BS), BF16),
            pltpu.VMEM((U, BS), F32),
            pltpu.VMEM((STEPS, U + 1, PAD + BS, BS), BF16),
            pltpu.VMEM((STEPS, 2, BS, BS), BF16),
            pltpu.VMEM((STEPS, U, BS, BS), BF16),
            pltpu.VMEM((U, BS, BS), BF16),
            dma((5,)),
            dma((2,)),
            dma((1,)),
            dma((STEPS, U + 1, PARTS)),
            dma((STEPS, U)),
            dma((U,)),
            dma((1,)),
        ],
        compiler_params=pltpu.CompilerParams(
            collective_id=0, has_side_effects=True, vmem_limit_bytes=VMEM_LIMIT),
    )(
        state.reshape(BS, flat // lanes, 1, lanes),
        coupling.reshape(BS, flat),
        coupling_t.reshape(coupling_t.shape[0], BS, flat),
        factor.reshape(U, SR, BS),
        cofactor.reshape(U, SR, BS),
        rates,
    )
    out = pl.pallas_call(
        store,
        out_shape=jax.ShapeDtypeStruct((BS, flat // lanes, 1, lanes), F32),
        in_specs=[vmem],
        out_specs=hbm,
        scratch_shapes=[dma((1,))],
        compiler_params=pltpu.CompilerParams(vmem_limit_bytes=2 * 1024 * 1024),
    )(work)
    return out.reshape(BS, 1, flat)


VMEM_LIMIT = 61 * 1024 * 1024


def solution(mesh):
    return jax.shard_map(
        on_device,
        mesh=mesh,
        in_specs=(
            P("row", "col", None),
            P("row", "col", None),
            P(None, "row", "col", None),
            P(None, "col", "row", None),
            P(None, "col", "row", None),
            P(None, "col", None),
        ),
        out_specs=P("row", "col", None),
        check_vma=False,
    )
```

```python
import functools

import jax
import jax.numpy as jnp
from jax import lax
from jax.experimental import pallas as pl
from jax.experimental.pallas import tpu as pltpu
from jax.sharding import PartitionSpec as P

STEPS = 2
PARTS = 4
PAD = 16
SAME = 2
HOME = False
MIX = True
RELAY = (False, False)
FORWARD = True
OP_MAX = 1.3
MESH = pl.DeviceIdType.MESH
F32 = jnp.float32
BF16 = jnp.bfloat16
NN = (((1,), (0,)), ((), ()))
NT = (((1,), (1,)), ((), ()))
scope = jax.named_scope


def halves(x):
    hi = x.astype(BF16)
    return hi, (x - hi.astype(F32)).astype(BF16)


def mm(a, b, dims):
    return lax.dot_general(a, b, dims, preferred_element_type=F32)


def dot3(a, b, dims):
    return mm(a[0], b[0], dims) + (mm(a[0], b[1], dims) + mm(a[1], b[0], dims))


def encode(x, inverse):
    v = jnp.exp2(jnp.sqrt(jnp.abs(x) * inverse) * 250.0 - 125.0)
    return jnp.where(x < 0, -v, v).astype(BF16)


def decode(v, scale):
    v = v.astype(F32)
    y = jnp.log2(jnp.abs(v)) * (1.0 / 250.0) + 0.5
    x = y * y * scale
    return jnp.where(v < 0, -x, x)


def kernel(R, C, U, BS, SR, state, upper_in, lower_in, factor, cofactor, rates_in, out,
           upper, lower, turned, raw, rates, enc, ops, mats, ebuf, xz, own, atb, an,
           load_sem, ops_sem, e_sem, xz_sem, at_sem, an_sem, send_sem):
    H = R // 2
    r = lax.axis_index("row")
    c = lax.axis_index("col")
    d = [2 * R - 1 - s for s in range(STEPS)]

    def owner(row, s):
        return (d[s] - row) % C

    o = [owner(r, s) for s in range(STEPS)]
    sends = []
    me = r * C + c

    barrier = pltpu.get_barrier_semaphore()

    pltpu.make_async_copy(cofactor, raw.at[0], load_sem.at[0]).start()
    pltpu.make_async_copy(factor, raw.at[1], load_sem.at[0]).start()

    @pl.loop(1, R * C)
    def _(k):
        peer = (me + k) % (R * C)
        pl.semaphore_signal(barrier, inc=1, device_id=(peer // C, peer % C), device_id_type=MESH)

    pltpu.make_async_copy(rates_in.at[:, 0, :], rates, load_sem.at[1]).start()
    pltpu.make_async_copy(lower_in, lower, load_sem.at[2]).start()
    lanes = out.shape[1] // state.shape[1]
    for j in range(state.shape[1]):
        pltpu.make_async_copy(state.at[:, j, 0, :], out.at[:, pl.ds(j * lanes, lanes)], load_sem.at[3]).start()
    pltpu.make_async_copy(upper_in, upper, load_sem.at[4]).start()

    def arrive(ref, sem):
        pltpu.make_async_copy(ref, ref, sem).wait()

    def send(cond, src, dst, sem, dev):
        copy = pltpu.make_async_remote_copy(
            src_ref=src, dst_ref=dst, send_sem=send_sem.at[0], recv_sem=sem,
            device_id=dev, device_id_type=MESH)
        sends.append((cond, copy, (src.shape, str(src.dtype))))

        @pl.when(cond)
        def _():
            copy.start()

    def send_or_local(cond, src, dst, sem, dev):
        mine = (dev[0] == r) & (dev[1] == c)
        send(cond & jnp.logical_not(mine), src, dst, sem, dev)

        @pl.when(cond & mine)
        def _():
            pltpu.make_async_copy(src, dst, sem).start()

    def slot(u):
        if isinstance(u, int):
            return pl.ds(u * BS, BS)
        return pl.ds(pl.multiple_of(u * BS, BS), BS)

    def target(row, m, s):
        return (row <= m) & (row + m < d[s])

    with scope("encode"):
        arrive(raw, load_sem.at[0])
        for u in range(U):
            both = jnp.concatenate([raw[0, u], raw[1, u]], axis=0)
            enc[u] = encode(both, 1.0 / OP_MAX)
        arrive(rates, load_sem.at[1])

    with scope("barrier"):
        pl.semaphore_wait(barrier, R * C - 1)

    def send_left(s):
        for u in range(U // 2):
            m = c + C * u
            send_or_local(m < R, enc.at[u], ops.at[0, r], ops_sem.at[0], (m, owner(m, s)))

    def send_right(s):
        for u in range(U // 2 - s, U):
            to = d[s] - (c + C * u)
            live = (to >= 0) & (to < R)
            if s > 0:
                live = live & (to % 4 == 3 if FORWARD else to % 2 == 1)
            send_or_local(live, enc.at[u], ops.at[1, r], ops_sem.at[1], (to, c))

    def send_lower(first):
        to = (r + H) % R
        top = (d[0] - 1 - to - c) // C
        for u in range(U - 1, -1, -1):
            m = c + C * u
            turn = u == top if first else u != top
            send(target(to, m, 0) & (m != to) & turn, lower.at[0, :, slot(u)], atb.at[0, u], at_sem.at[0, u], (to, c))

    def send_middle():
        for u in range(U):
            m = c + C * u
            send((r == 0) & (m >= H) & target(H - 1, m, 1), lower.at[0, :, slot(u)], atb.at[1, u],
                 at_sem.at[1, u], (H - 1, c))

    q1 = (d[1] - r) // C
    first = c == o[1]
    top = (d[0] - 1 - r - c) // C
    ahead = c != o[0]

    def needs(u):
        m = c + C * u
        return target(r, m, 0) & (m != r)

    def picked(u):
        return first & (q1 == u)

    def crossing(i, m):
        beside = ((m + 1 + H) % R) // 2 == i // 2
        same = (m - i) % C == 0
        return (m % C == C - 1) | (same & beside if SAME == 1 else same if SAME else False)

    def send_turned(cond):
        for t in range(2):
            m = (r + H) % R + R * t - 1
            for u in range(U // 2):
                i = c + C * u
                live = cond & (m >= 0) & target(i, m, 1) & crossing(i, m)
                to_u = jnp.clip(m // C, 0, U - 1)
                mine = (i == r) & (m % C == c)
                k = t * (U // 2) + u

                @pl.when(live)
                def _(t=t, u=u, k=k):
                    turned[k] = jnp.transpose(lower[t, :, slot(u)])

                send(live & jnp.logical_not(mine), turned.at[k], an.at[to_u], an_sem.at[to_u], (i, m % C))

                @pl.when(live & mine)
                def _(k=k, to_u=to_u):
                    pltpu.make_async_copy(turned.at[k], an.at[to_u], an_sem.at[to_u]).start()

    def send_upper(cond, held=None):
        late = first & (r % 2 == 0)
        for u in range(U):
            m = c + C * u - 1
            to = (c + C - 1) % C
            to_u = jnp.maximum(jnp.where(c >= 1, u, u - 1), 0)
            if u >= U // 2:
                now = late if held else cond & jnp.logical_not(late)
            elif held:
                continue
            else:
                now = cond
            send(now & jnp.logical_not(crossing(r, m)) & (m >= 0) & target(r, m, 1), upper.at[:, slot(u)], an.at[to_u],
                 an_sem.at[to_u], (r, to))

    def hand_down(u):
        m = c + C * u
        live = (r >= 1) & (r != H) & (m >= r) & target(r - 1, m, 1)
        to = (jnp.maximum(r - 1, 0), c)
        send(live, atb.at[0, u], atb.at[1, u], at_sem.at[1, u], to)

    with scope("sends0"):
        send_left(0)
        send_right(0)
        for s in range(STEPS):
            send_or_local(c == r % C, rates, ebuf, e_sem.at[0], (r, o[s]))
        send_left(1)
        arrive(lower, load_sem.at[2])
        send_lower(True)
        send_right(1)
        send_lower(False)
        send_middle()
        arrive(upper, load_sem.at[4])
        arrive(out, load_sem.at[3])
        send_upper(c != o[0])

    with scope("gate"):
        @pl.when(ahead & needs(top))
        def _():
            arrive(atb.at[0, top], at_sem.at[0, top])

        send_turned(c != o[0])
        for u in range(U // 2):
            @pl.when(target(r, c + C * u, 0) & (c + C * u == r))
            def _(u=u):
                atb[0, u] = jnp.transpose(upper[:, slot(u)])

    half = BS // PARTS

    def part(h):
        if h == 0:
            return pl.ds(0, PAD + half)
        return pl.ds(PAD + h * half, half)

    def spread(s, h, who):
        home = r % C
        own_col = home == c
        k = jnp.where(own_col, r // C, (d[s] - r) // C)
        straight = home == 0 if s > 0 and HOME else False
        has = (own_col & jnp.logical_not(straight) | (c == o[s])) & who

        def give(cond, to):
            if s > 0 and HOME:
                send(cond & who & straight & (c == o[s]) & (home != c), xz.at[s, U, part(h)],
                     xz.at[s, r // C, part(h)], xz_sem.at[s, r // C, h], (to, home))
            send(cond & has, xz.at[s, U, part(h)], xz.at[s, k, part(h)], xz_sem.at[s, k, h], (to, c))

        give(r % 2 == 1, jnp.maximum(r - 1, 0))
        for back in range(R // 2 - 1, 0, -1) if s > 0 and HOME else range(1, R // 2):
            if back == 3 and RELAY[s]:
                continue
            pair = r // 2 - back
            give(pair >= 0, jnp.maximum(2 * pair + 1 - r % 2, 0))

    def wants(col, s):
        return (col - r) % C < d[s] - 2 * r

    def give_row(s):
        at = c == o[s]
        home = r % C
        goal = (o[s] + C - 1) % C
        def give(cond, to):
            for h in range(PARTS):
                block = xz.at[s, U, part(h)]
                send(at & cond, block, block, xz_sem.at[s, U, h], (r, jnp.clip(to, 0, C - 1)))

        give(True if s == 0 else home != c, goal if s == 0 else home)
        for h in range(PARTS):
            spread(s, h, at)
        if s == 0:
            give((home != c) & (home != goal), home)
        for far_by in range(C - 1, 0, -1):
            for to in (c - far_by, c + far_by):
                live = (to >= 0) & (to < C) & (to != home) & wants(to, s)
                if s == 0:
                    live = live & (to != goal)
                give(live, to)

    def take_row(s):
        other = (c != o[s]) & (wants(c, s) | (c == r % C))
        if s == 0:
            other = other | first
        for h in range(PARTS):
            block = xz.at[s, U, part(h)]
            sem = xz_sem.at[s, U, h]

            @pl.when(other)
            def _(block=block, sem=sem):
                arrive(block, sem)

            spread(s, h, other)

    def decoded(s, k):
        return decode(xz[s, k, PAD:], xz[s, k, 0:1, :].astype(F32))

    def split_own(s):
        xh, xl = halves(decoded(s, U))
        own[s, 0] = xh
        own[s, 1] = xl

    def prepare(s):
        with scope("w_e"):
            arrive(ebuf, e_sem.at[0])
        group = max(1, 16 // SR)
        for side in range(2):
            with scope("w_op%d" % side):
                arrive(ops.at[side], ops_sem.at[side])
            if s == 0 and side == 1:
                pl.when(hands)(hand_right.start)
            for k in range(0, R, group):
                both = [decode(ops[side, k + i], OP_MAX) for i in range(group)]
                for which in range(2):
                    rows = [b[which * SR:(which + 1) * SR] for b in both]
                    hi, lo = halves(rows[0] if group == 1 else jnp.concatenate(rows, axis=0))
                    mats[2 * side + which, 0, k * SR:(k + group) * SR] = hi
                    mats[2 * side + which, 1, k * SR:(k + group) * SR] = lo

    def solve(s):
        q = (d[s] - r) // C
        left_e = jnp.transpose(jnp.broadcast_to(ebuf[pl.ds(r // C, 1), :], (BS, BS)))
        rate = left_e + rates[pl.ds(q, 1), :]
        mat = [(mats[k, 0], mats[k, 1]) for k in range(4)]
        mid = dot3(mat[0], halves(out[:, slot(q)]), NN)
        mid = dot3(halves(mid), mat[2], NT) / rate
        mid = dot3(mat[1], halves(mid), NN)
        x = -dot3(halves(mid), mat[3], NT)
        out[:, slot(q)] = x
        peak = jnp.max(jnp.abs(x), axis=0, keepdims=True) * 1.01 + 1e-30
        scale = peak.astype(BF16)
        xz[s, U, :PAD] = jnp.broadcast_to(scale, (PAD, BS))
        xz[s, U, PAD:] = encode(x, 1.0 / scale.astype(F32))

    def z_index(u, s):
        m = c + C * u
        j = jnp.where(d[s] - m <= m, d[s] - m, m)
        k = jnp.where(j == r, U, jnp.where(j % C == c, j // C, u))
        return j, k

    def collect(u, s, direct, extra=True):
        j, k = z_index(u, s)
        crossed = (r // 2 < j // 2) & (r % 2 != j % 2)
        landed = (r < j) & (crossed if direct else jnp.logical_not(crossed))
        if u >= U // 2:
            landed = landed & (j % C != c)
        landed = landed & extra

        for h in range(PARTS):
            block = xz.at[s, u, part(h)]

            @pl.when(landed)
            def _(block=block, h=h):
                arrive(block, xz_sem.at[s, u, h])

            if direct:
                send(landed, block, block, xz_sem.at[s, u, h], (r + 1 - 2 * (r % 2), c))
                if RELAY[s]:
                    on = landed & (r // 2 >= 1) & (j // 2 - r // 2 == 2)
                    send(on, block, block, xz_sem.at[s, u, h], (jnp.maximum(r - 2, 0), c))

    def update(u, s):
        m = c + C * u
        j, k = z_index(u, s)

        if s > 0:
            @pl.when(m != r)
            def _():
                arrive(atb.at[s, u], at_sem.at[s, u])

        def apply(dims):
            a = an[u] if s > 0 else upper[:, slot(u)]
            zh, zl = halves(decoded(s, k))
            row = mm(own[s, 0], atb[s, u], NN) + mm(own[s, 1], atb[s, u], NN)
            out[:, slot(u)] -= row + (mm(a, zh, dims) + mm(a, zl, dims))

        low, high = C * u, C * u + C - 1
        if 2 * low >= d[s]:
            apply(NN)
        elif 2 * high < d[s]:
            apply(NT)
        else:
            straight = d[s] - m <= m
            pl.when(straight)(lambda: apply(NN))
            pl.when(jnp.logical_not(straight))(lambda: apply(NT))

    hand_right = pltpu.make_async_remote_copy(
        src_ref=ops.at[1], dst_ref=ops.at[1], send_sem=send_sem.at[0], recv_sem=ops_sem.at[1],
        device_id=(jnp.maximum(r - 1, 0), c), device_id_type=MESH)
    hands = r % 4 != 0 if FORWARD else r % 2 == 1
    sends.append(((c == o[0]) & hands, hand_right, ops.at[1].shape))

    @pl.when(c == o[0])
    def _():
        with scope("solve0"):
            prepare(0)
            solve(0)

    with scope("give0"):
        give_row(0)
        send_upper(c == o[0])
        send_turned(c == o[0])

    @pl.when(first)
    def _():
        with scope("prep"):
            prepare(1)

    with scope("take0"):
        take_row(0)
        pl.when(wants(c, 0) | first)(lambda: split_own(0))

    with scope("pick0"):
        for u in range(U // 2 - 1, U):
            collect(u, 0, True, picked(u))
            collect(u, 0, False, picked(u))

            @pl.when(picked(u))
            def _(u=u):
                update(u, 0)

    @pl.when(first)
    def _():
        with scope("solve1"):
            solve(1)

    with scope("give1"):
        give_row(1)
        send_upper(None, True)

    def at_hand(u, s):
        j, k = z_index(u, s)
        return (j == r) | ((r // 2 < j // 2) & (r % 2 != j % 2))

    def use(s, u, here, also=True):
        live = also & target(r, c + C * u, s) & (at_hand(u, s) if here else jnp.logical_not(at_hand(u, s)))
        if s == 0:
            live = live & jnp.logical_not(picked(u))
        pl.when(live)(lambda: update(u, s))

    with scope("direct0"):
        for u in range(U - 1, -1, -1):
            collect(u, 0, True, jnp.logical_not(picked(u)))
    with scope("hand"):
        for u in range(U - 1, -1, -1):
            @pl.when(needs(u) & jnp.logical_not(ahead & (top == u)))
            def _(u=u):
                arrive(atb.at[0, u], at_sem.at[0, u])

            hand_down(u)
    with scope("A0"):
        for u in range(U):
            use(0, u, True)
    with scope("B0"):
        for u in range(U - 1, -1, -1):
            collect(u, 0, False, jnp.logical_not(picked(u)))
            use(0, u, False)

    def twice(u):
        j, k = z_index(u, 1)
        return (u >= U // 2) & (j % C == c)

    with scope("take1"):
        take_row(1)
        pl.when(wants(c, 1))(lambda: split_own(1))
    if not MIX:
        for u in range(U - 1, -1, -1):
            collect(u, 1, True)
    with scope("w_an"):
        for u in range(U):
            m = c + C * u

            @pl.when(target(r, m, 1))
            def _(u=u):
                arrive(an.at[u], an_sem.at[u])

            if u < U // 2:
                @pl.when(target(r, m, 1) & (m == r))
                def _(u=u):
                    atb[1, u] = jnp.transpose(an[u])
    if MIX:
        for u in range(U - 1, -1, -1):
            with scope("direct1_%d" % u):
                collect(u, 1, True)
            with scope("A1_%d" % u):
                use(1, u, True, jnp.logical_not(twice(u)))
    with scope("A1"):
        for u in range(U):
            if MIX and u < U // 2:
                continue
            use(1, u, True, twice(u) if MIX else True)
    with scope("drain"):
        sizes = {}
        for cond, copy, size in sends:
            sizes.setdefault(size, []).append((cond, copy))
        for group in sizes.values():
            count = sum(jnp.where(cond, 1, 0) for cond, _ in group)

            @pl.loop(0, count)
            def _(_, copy=group[0][1]):
                copy.wait_send()
    for u in range(U - 1, -1, -1):
        with scope("B1_%d" % u):
            collect(u, 1, False)
            use(1, u, False, jnp.logical_not(twice(u)))
    for u in range(U // 2, U):
        with scope("C1_%d" % u):
            use(1, u, False, twice(u))


def store(work, out, sem):
    lanes = work.shape[1] // out.shape[1]
    for j in range(out.shape[1]):
        pltpu.make_async_copy(work.at[:, pl.ds(j * lanes, lanes)], out.at[:, j, 0, :], sem.at[0]).start()
    pltpu.make_async_copy(work, work, sem.at[0]).wait()


def on_device(state, coupling, coupling_t, factor, cofactor, rates):
    R = lax.axis_size("row")
    C = lax.axis_size("col")
    U = 2 * R // C
    BS = state.shape[0]
    SR = factor.shape[2]
    flat = U * BS
    lanes = 128
    vmem = pl.BlockSpec(memory_space=pltpu.VMEM)
    hbm = pl.BlockSpec(memory_space=pltpu.HBM)
    dma = pltpu.SemaphoreType.DMA
    work = pl.pallas_call(
        functools.partial(kernel, R, C, U, BS, SR),
        out_shape=pltpu.VMEM((BS, flat), F32),
        in_specs=[hbm] * 6,
        out_specs=vmem,
        scratch_shapes=[
            pltpu.VMEM((BS, flat), BF16),
            pltpu.VMEM((2, BS, flat), BF16),
            pltpu.VMEM((U, BS, BS), BF16),
            pltpu.VMEM((2, U, SR, BS), F32),
            pltpu.VMEM((U, BS), F32),
            pltpu.VMEM((U, 2 * SR, BS), BF16),
            pltpu.VMEM((2, R, 2 * SR, BS), BF16),
            pltpu.VMEM((4, 2, BS, BS), BF16),
            pltpu.VMEM((U, BS), F32),
            pltpu.VMEM((STEPS, U + 1, PAD + BS, BS), BF16),
            pltpu.VMEM((STEPS, 2, BS, BS), BF16),
            pltpu.VMEM((STEPS, U, BS, BS), BF16),
            pltpu.VMEM((U, BS, BS), BF16),
            dma((5,)),
            dma((2,)),
            dma((1,)),
            dma((STEPS, U + 1, PARTS)),
            dma((STEPS, U)),
            dma((U,)),
            dma((1,)),
        ],
        compiler_params=pltpu.CompilerParams(
            collective_id=0, has_side_effects=True, vmem_limit_bytes=VMEM_LIMIT),
    )(
        state.reshape(BS, flat // lanes, 1, lanes),
        coupling.reshape(BS, flat),
        coupling_t.reshape(coupling_t.shape[0], BS, flat),
        factor.reshape(U, SR, BS),
        cofactor.reshape(U, SR, BS),
        rates,
    )
    out = pl.pallas_call(
        store,
        out_shape=jax.ShapeDtypeStruct((BS, flat // lanes, 1, lanes), F32),
        in_specs=[vmem],
        out_specs=hbm,
        scratch_shapes=[dma((1,))],
        compiler_params=pltpu.CompilerParams(vmem_limit_bytes=2 * 1024 * 1024),
    )(work)
    return out.reshape(BS, 1, flat)


VMEM_LIMIT = 61 * 1024 * 1024


def solution(mesh):
    return jax.shard_map(
        on_device,
        mesh=mesh,
        in_specs=(
            P("row", "col", None),
            P("row", "col", None),
            P(None, "row", "col", None),
            P(None, "col", "row", None),
            P(None, "col", "row", None),
            P(None, "col", None),
        ),
        out_specs=P("row", "col", None),
        check_vma=False,
    )
```

```python
import functools

import jax
import jax.numpy as jnp
from jax import lax
from jax.experimental import pallas as pl
from jax.experimental.pallas import tpu as pltpu
from jax.sharding import PartitionSpec as P

STEPS = 2
PARTS = 4
PAD = 16
SAME = 2
HOME = False
MIX = True
RELAY = (False, False)
FORWARD = True
OP_MAX = 1.3
MESH = pl.DeviceIdType.MESH
F32 = jnp.float32
BF16 = jnp.bfloat16
NN = (((1,), (0,)), ((), ()))
NT = (((1,), (1,)), ((), ()))
scope = jax.named_scope


def halves(x):
    hi = x.astype(BF16)
    return hi, (x - hi.astype(F32)).astype(BF16)


def mm(a, b, dims):
    return lax.dot_general(a, b, dims, preferred_element_type=F32)


def dot3(a, b, dims):
    return mm(a[0], b[0], dims) + (mm(a[0], b[1], dims) + mm(a[1], b[0], dims))


def encode(x, inverse):
    v = jnp.exp2(jnp.sqrt(jnp.abs(x) * inverse) * 250.0 - 125.0)
    return jnp.where(x < 0, -v, v).astype(BF16)


def decode(v, scale):
    v = v.astype(F32)
    y = jnp.log2(jnp.abs(v)) * (1.0 / 250.0) + 0.5
    x = y * y * scale
    return jnp.where(v < 0, -x, x)


def kernel(R, C, U, BS, SR, state, upper_in, lower_in, factor, cofactor, rates_in, out,
           upper, lower, turned, raw, rates, enc, ops, mats, ebuf, xz, own, atb, an,
           load_sem, ops_sem, e_sem, xz_sem, at_sem, an_sem, send_sem):
    H = R // 2
    r = lax.axis_index("row")
    c = lax.axis_index("col")
    d = [2 * R - 1 - s for s in range(STEPS)]

    def owner(row, s):
        return (d[s] - row) % C

    o = [owner(r, s) for s in range(STEPS)]
    sends = []
    me = r * C + c

    barrier = pltpu.get_barrier_semaphore()

    pltpu.make_async_copy(cofactor, raw.at[0], load_sem.at[0]).start()
    pltpu.make_async_copy(factor, raw.at[1], load_sem.at[0]).start()

    @pl.loop(1, R * C)
    def _(k):
        peer = (me + k) % (R * C)
        pl.semaphore_signal(barrier, inc=1, device_id=(peer // C, peer % C), device_id_type=MESH)

    pltpu.make_async_copy(rates_in.at[:, 0, :], rates, load_sem.at[1]).start()
    pltpu.make_async_copy(lower_in, lower, load_sem.at[2]).start()
    lanes = out.shape[1] // state.shape[1]
    for j in range(state.shape[1]):
        pltpu.make_async_copy(state.at[:, j, 0, :], out.at[:, pl.ds(j * lanes, lanes)], load_sem.at[3]).start()
    pltpu.make_async_copy(upper_in, upper, load_sem.at[4]).start()

    def arrive(ref, sem):
        pltpu.make_async_copy(ref, ref, sem).wait()

    def send(cond, src, dst, sem, dev):
        copy = pltpu.make_async_remote_copy(
            src_ref=src, dst_ref=dst, send_sem=send_sem.at[0], recv_sem=sem,
            device_id=dev, device_id_type=MESH)
        sends.append((cond, copy, (src.shape, str(src.dtype))))

        @pl.when(cond)
        def _():
            copy.start()

    def send_or_local(cond, src, dst, sem, dev):
        mine = (dev[0] == r) & (dev[1] == c)
        send(cond & jnp.logical_not(mine), src, dst, sem, dev)

        @pl.when(cond & mine)
        def _():
            pltpu.make_async_copy(src, dst, sem).start()

    def slot(u):
        if isinstance(u, int):
            return pl.ds(u * BS, BS)
        return pl.ds(pl.multiple_of(u * BS, BS), BS)

    def target(row, m, s):
        return (row <= m) & (row + m < d[s])

    with scope("encode"):
        arrive(raw, load_sem.at[0])
        for u in range(U):
            both = jnp.concatenate([raw[0, u], raw[1, u]], axis=0)
            enc[u] = encode(both, 1.0 / OP_MAX)
        arrive(rates, load_sem.at[1])

    with scope("barrier"):
        pl.semaphore_wait(barrier, R * C - 1)

    def send_left(s):
        for u in range(U // 2 - 1, -1, -1):
            m = c + C * u
            send_or_local(m < R, enc.at[u], ops.at[0, r], ops_sem.at[0], (m, owner(m, s)))

    def send_right(s):
        for u in range(U // 2 - s, U):
            to = d[s] - (c + C * u)
            live = (to >= 0) & (to < R)
            if s > 0:
                live = live & (to % 4 == 3 if FORWARD else to % 2 == 1)
            send_or_local(live, enc.at[u], ops.at[1, r], ops_sem.at[1], (to, c))

    def send_lower(first):
        to = (r + H) % R
        top = (d[0] - 1 - to - c) // C
        for u in range(U - 1, -1, -1):
            m = c + C * u
            turn = u == top if first else u != top
            send(target(to, m, 0) & (m != to) & turn, lower.at[0, :, slot(u)], atb.at[0, u], at_sem.at[0, u], (to, c))

    def send_middle():
        for u in range(U):
            m = c + C * u
            send((r == 0) & (m >= H) & target(H - 1, m, 1), lower.at[0, :, slot(u)], atb.at[1, u],
                 at_sem.at[1, u], (H - 1, c))

    q1 = (d[1] - r) // C
    first = c == o[1]
    top = (d[0] - 1 - r - c) // C
    ahead = c != o[0]

    def needs(u):
        m = c + C * u
        return target(r, m, 0) & (m != r)

    def picked(u):
        return first & (q1 == u)

    def crossing(i, m):
        beside = ((m + 1 + H) % R) // 2 == i // 2
        same = (m - i) % C == 0
        return (m % C == C - 1) | (same & beside if SAME == 1 else same if SAME else False)

    def send_turned(cond):
        for t in range(2):
            m = (r + H) % R + R * t - 1
            for u in range(U // 2):
                i = c + C * u
                live = cond & (m >= 0) & target(i, m, 1) & crossing(i, m)
                to_u = jnp.clip(m // C, 0, U - 1)
                mine = (i == r) & (m % C == c)
                k = t * (U // 2) + u

                @pl.when(live)
                def _(t=t, u=u, k=k):
                    turned[k] = jnp.transpose(lower[t, :, slot(u)])

                send(live & jnp.logical_not(mine), turned.at[k], an.at[to_u], an_sem.at[to_u], (i, m % C))

                @pl.when(live & mine)
                def _(k=k, to_u=to_u):
                    pltpu.make_async_copy(turned.at[k], an.at[to_u], an_sem.at[to_u]).start()

    def send_upper(cond, held=None):
        late = first & (r % 2 == 0)
        for u in range(U):
            m = c + C * u - 1
            to = (c + C - 1) % C
            to_u = jnp.maximum(jnp.where(c >= 1, u, u - 1), 0)
            if u >= U // 2:
                now = late if held else cond & jnp.logical_not(late)
            elif held:
                continue
            else:
                now = cond
            send(now & jnp.logical_not(crossing(r, m)) & (m >= 0) & target(r, m, 1), upper.at[:, slot(u)], an.at[to_u],
                 an_sem.at[to_u], (r, to))

    def hand_down(u):
        m = c + C * u
        live = (r >= 1) & (r != H) & (m >= r) & target(r - 1, m, 1)
        to = (jnp.maximum(r - 1, 0), c)
        send(live, atb.at[0, u], atb.at[1, u], at_sem.at[1, u], to)

    with scope("sends0"):
        send_left(0)
        send_right(0)
        for s in range(STEPS):
            send_or_local(c == r % C, rates, ebuf, e_sem.at[0], (r, o[s]))
        send_left(1)
        arrive(lower, load_sem.at[2])
        send_lower(True)
        send_right(1)
        send_lower(False)
        send_middle()
        arrive(upper, load_sem.at[4])
        arrive(out, load_sem.at[3])
        send_upper(c != o[0])

    with scope("gate"):
        @pl.when(ahead & needs(top))
        def _():
            arrive(atb.at[0, top], at_sem.at[0, top])

        send_turned(c != o[0])
        for u in range(U // 2):
            @pl.when(target(r, c + C * u, 0) & (c + C * u == r))
            def _(u=u):
                atb[0, u] = jnp.transpose(upper[:, slot(u)])

    half = BS // PARTS

    def part(h):
        if h == 0:
            return pl.ds(0, PAD + half)
        return pl.ds(PAD + h * half, half)

    def spread(s, h, who):
        home = r % C
        own_col = home == c
        k = jnp.where(own_col, r // C, (d[s] - r) // C)
        straight = home == 0 if s > 0 and HOME else False
        has = (own_col & jnp.logical_not(straight) | (c == o[s])) & who

        def give(cond, to):
            if s > 0 and HOME:
                send(cond & who & straight & (c == o[s]) & (home != c), xz.at[s, U, part(h)],
                     xz.at[s, r // C, part(h)], xz_sem.at[s, r // C, h], (to, home))
            send(cond & has, xz.at[s, U, part(h)], xz.at[s, k, part(h)], xz_sem.at[s, k, h], (to, c))

        give(r % 2 == 1, jnp.maximum(r - 1, 0))
        for back in range(R // 2 - 1, 0, -1) if s > 0 and HOME else range(1, R // 2):
            if back == 3 and RELAY[s]:
                continue
            pair = r // 2 - back
            give(pair >= 0, jnp.maximum(2 * pair + 1 - r % 2, 0))

    def wants(col, s):
        return (col - r) % C < d[s] - 2 * r

    def give_row(s):
        at = c == o[s]
        home = r % C
        goal = (o[s] + C - 1) % C
        def give(cond, to):
            for h in range(PARTS):
                block = xz.at[s, U, part(h)]
                send(at & cond, block, block, xz_sem.at[s, U, h], (r, jnp.clip(to, 0, C - 1)))

        give(True if s == 0 else home != c, goal if s == 0 else home)
        for h in range(PARTS):
            spread(s, h, at)
        if s == 0:
            give((home != c) & (home != goal), home)
        for far_by in range(C - 1, 0, -1):
            for to in (c - far_by, c + far_by):
                live = (to >= 0) & (to < C) & (to != home) & wants(to, s)
                if s == 0:
                    live = live & (to != goal)
                give(live, to)

    def take_row(s):
        other = (c != o[s]) & (wants(c, s) | (c == r % C))
        if s == 0:
            other = other | first
        for h in range(PARTS):
            block = xz.at[s, U, part(h)]
            sem = xz_sem.at[s, U, h]

            @pl.when(other)
            def _(block=block, sem=sem):
                arrive(block, sem)

            spread(s, h, other)

    def decoded(s, k):
        return decode(xz[s, k, PAD:], xz[s, k, 0:1, :].astype(F32))

    def split_own(s):
        xh, xl = halves(decoded(s, U))
        own[s, 0] = xh
        own[s, 1] = xl

    def prepare(s):
        with scope("w_e"):
            arrive(ebuf, e_sem.at[0])
        group = max(1, 16 // SR)
        for side in range(2):
            with scope("w_op%d" % side):
                arrive(ops.at[side], ops_sem.at[side])
            if s == 0 and side == 1:
                pl.when(hands)(hand_right.start)
            for k in range(0, R, group):
                both = [decode(ops[side, k + i], OP_MAX) for i in range(group)]
                for which in range(2):
                    rows = [b[which * SR:(which + 1) * SR] for b in both]
                    hi, lo = halves(rows[0] if group == 1 else jnp.concatenate(rows, axis=0))
                    mats[2 * side + which, 0, k * SR:(k + group) * SR] = hi
                    mats[2 * side + which, 1, k * SR:(k + group) * SR] = lo

    def solve(s):
        q = (d[s] - r) // C
        left_e = jnp.transpose(jnp.broadcast_to(ebuf[pl.ds(r // C, 1), :], (BS, BS)))
        rate = left_e + rates[pl.ds(q, 1), :]
        mat = [(mats[k, 0], mats[k, 1]) for k in range(4)]
        mid = dot3(mat[0], halves(out[:, slot(q)]), NN)
        mid = dot3(halves(mid), mat[2], NT) / rate
        mid = dot3(mat[1], halves(mid), NN)
        x = -dot3(halves(mid), mat[3], NT)
        out[:, slot(q)] = x
        peak = jnp.max(jnp.abs(x), axis=0, keepdims=True) * 1.01 + 1e-30
        scale = peak.astype(BF16)
        xz[s, U, :PAD] = jnp.broadcast_to(scale, (PAD, BS))
        xz[s, U, PAD:] = encode(x, 1.0 / scale.astype(F32))

    def z_index(u, s):
        m = c + C * u
        j = jnp.where(d[s] - m <= m, d[s] - m, m)
        k = jnp.where(j == r, U, jnp.where(j % C == c, j // C, u))
        return j, k

    def collect(u, s, direct, extra=True):
        j, k = z_index(u, s)
        crossed = (r // 2 < j // 2) & (r % 2 != j % 2)
        landed = (r < j) & (crossed if direct else jnp.logical_not(crossed))
        if u >= U // 2:
            landed = landed & (j % C != c)
        landed = landed & extra

        for h in range(PARTS):
            block = xz.at[s, u, part(h)]

            @pl.when(landed)
            def _(block=block, h=h):
                arrive(block, xz_sem.at[s, u, h])

            if direct:
                send(landed, block, block, xz_sem.at[s, u, h], (r + 1 - 2 * (r % 2), c))
                if RELAY[s]:
                    on = landed & (r // 2 >= 1) & (j // 2 - r // 2 == 2)
                    send(on, block, block, xz_sem.at[s, u, h], (jnp.maximum(r - 2, 0), c))

    def update(u, s):
        m = c + C * u
        j, k = z_index(u, s)

        if s > 0:
            @pl.when(m != r)
            def _():
                arrive(atb.at[s, u], at_sem.at[s, u])

        def apply(dims):
            a = an[u] if s > 0 else upper[:, slot(u)]
            zh, zl = halves(decoded(s, k))
            row = mm(own[s, 0], atb[s, u], NN) + mm(own[s, 1], atb[s, u], NN)
            out[:, slot(u)] -= row + (mm(a, zh, dims) + mm(a, zl, dims))

        low, high = C * u, C * u + C - 1
        if 2 * low >= d[s]:
            apply(NN)
        elif 2 * high < d[s]:
            apply(NT)
        else:
            straight = d[s] - m <= m
            pl.when(straight)(lambda: apply(NN))
            pl.when(jnp.logical_not(straight))(lambda: apply(NT))

    hand_right = pltpu.make_async_remote_copy(
        src_ref=ops.at[1], dst_ref=ops.at[1], send_sem=send_sem.at[0], recv_sem=ops_sem.at[1],
        device_id=(jnp.maximum(r - 1, 0), c), device_id_type=MESH)
    hands = r % 4 != 0 if FORWARD else r % 2 == 1
    sends.append(((c == o[0]) & hands, hand_right, ops.at[1].shape))

    @pl.when(c == o[0])
    def _():
        with scope("solve0"):
            prepare(0)
            solve(0)

    with scope("give0"):
        give_row(0)
        send_upper(c == o[0])
        send_turned(c == o[0])

    @pl.when(first)
    def _():
        with scope("prep"):
            prepare(1)

    with scope("take0"):
        take_row(0)
        pl.when(wants(c, 0) | first)(lambda: split_own(0))

    with scope("pick0"):
        for u in range(U // 2 - 1, U):
            collect(u, 0, True, picked(u))
            collect(u, 0, False, picked(u))

            @pl.when(picked(u))
            def _(u=u):
                update(u, 0)

    @pl.when(first)
    def _():
        with scope("solve1"):
            solve(1)

    with scope("give1"):
        give_row(1)
        send_upper(None, True)

    def at_hand(u, s):
        j, k = z_index(u, s)
        return (j == r) | ((r // 2 < j // 2) & (r % 2 != j % 2))

    def use(s, u, here, also=True):
        live = also & target(r, c + C * u, s) & (at_hand(u, s) if here else jnp.logical_not(at_hand(u, s)))
        if s == 0:
            live = live & jnp.logical_not(picked(u))
        pl.when(live)(lambda: update(u, s))

    with scope("direct0"):
        for u in range(U - 1, -1, -1):
            collect(u, 0, True, jnp.logical_not(picked(u)))
    with scope("hand"):
        for u in range(U - 1, -1, -1):
            @pl.when(needs(u) & jnp.logical_not(ahead & (top == u)))
            def _(u=u):
                arrive(atb.at[0, u], at_sem.at[0, u])

            hand_down(u)
    with scope("A0"):
        for u in range(U):
            use(0, u, True)
    with scope("B0"):
        for u in range(U - 1, -1, -1):
            collect(u, 0, False, jnp.logical_not(picked(u)))
            use(0, u, False)

    def twice(u):
        j, k = z_index(u, 1)
        return (u >= U // 2) & (j % C == c)

    with scope("take1"):
        take_row(1)
        pl.when(wants(c, 1))(lambda: split_own(1))
    if not MIX:
        for u in range(U - 1, -1, -1):
            collect(u, 1, True)
    with scope("w_an"):
        for u in range(U):
            m = c + C * u

            @pl.when(target(r, m, 1))
            def _(u=u):
                arrive(an.at[u], an_sem.at[u])

            if u < U // 2:
                @pl.when(target(r, m, 1) & (m == r))
                def _(u=u):
                    atb[1, u] = jnp.transpose(an[u])
    if MIX:
        for u in range(U - 1, -1, -1):
            with scope("direct1_%d" % u):
                collect(u, 1, True)
            with scope("A1_%d" % u):
                use(1, u, True, jnp.logical_not(twice(u)))
    with scope("A1"):
        for u in range(U):
            if MIX and u < U // 2:
                continue
            use(1, u, True, twice(u) if MIX else True)
    with scope("drain"):
        sizes = {}
        for cond, copy, size in sends:
            sizes.setdefault(size, []).append((cond, copy))
        for group in sizes.values():
            count = sum(jnp.where(cond, 1, 0) for cond, _ in group)

            @pl.loop(0, count)
            def _(_, copy=group[0][1]):
                copy.wait_send()
    for u in range(U - 1, -1, -1):
        with scope("B1_%d" % u):
            collect(u, 1, False)
            use(1, u, False, jnp.logical_not(twice(u)))
    for u in range(U // 2, U):
        with scope("C1_%d" % u):
            use(1, u, False, twice(u))


def store(work, out, sem):
    lanes = work.shape[1] // out.shape[1]
    for j in range(out.shape[1]):
        pltpu.make_async_copy(work.at[:, pl.ds(j * lanes, lanes)], out.at[:, j, 0, :], sem.at[0]).start()
    pltpu.make_async_copy(work, work, sem.at[0]).wait()


def on_device(state, coupling, coupling_t, factor, cofactor, rates):
    R = lax.axis_size("row")
    C = lax.axis_size("col")
    U = 2 * R // C
    BS = state.shape[0]
    SR = factor.shape[2]
    flat = U * BS
    lanes = 128
    vmem = pl.BlockSpec(memory_space=pltpu.VMEM)
    hbm = pl.BlockSpec(memory_space=pltpu.HBM)
    dma = pltpu.SemaphoreType.DMA
    work = pl.pallas_call(
        functools.partial(kernel, R, C, U, BS, SR),
        out_shape=pltpu.VMEM((BS, flat), F32),
        in_specs=[hbm] * 6,
        out_specs=vmem,
        scratch_shapes=[
            pltpu.VMEM((BS, flat), BF16),
            pltpu.VMEM((2, BS, flat), BF16),
            pltpu.VMEM((U, BS, BS), BF16),
            pltpu.VMEM((2, U, SR, BS), F32),
            pltpu.VMEM((U, BS), F32),
            pltpu.VMEM((U, 2 * SR, BS), BF16),
            pltpu.VMEM((2, R, 2 * SR, BS), BF16),
            pltpu.VMEM((4, 2, BS, BS), BF16),
            pltpu.VMEM((U, BS), F32),
            pltpu.VMEM((STEPS, U + 1, PAD + BS, BS), BF16),
            pltpu.VMEM((STEPS, 2, BS, BS), BF16),
            pltpu.VMEM((STEPS, U, BS, BS), BF16),
            pltpu.VMEM((U, BS, BS), BF16),
            dma((5,)),
            dma((2,)),
            dma((1,)),
            dma((STEPS, U + 1, PARTS)),
            dma((STEPS, U)),
            dma((U,)),
            dma((1,)),
        ],
        compiler_params=pltpu.CompilerParams(
            collective_id=0, has_side_effects=True, vmem_limit_bytes=VMEM_LIMIT),
    )(
        state.reshape(BS, flat // lanes, 1, lanes),
        coupling.reshape(BS, flat),
        coupling_t.reshape(coupling_t.shape[0], BS, flat),
        factor.reshape(U, SR, BS),
        cofactor.reshape(U, SR, BS),
        rates,
    )
    out = pl.pallas_call(
        store,
        out_shape=jax.ShapeDtypeStruct((BS, flat // lanes, 1, lanes), F32),
        in_specs=[vmem],
        out_specs=hbm,
        scratch_shapes=[dma((1,))],
        compiler_params=pltpu.CompilerParams(vmem_limit_bytes=2 * 1024 * 1024),
    )(work)
    return out.reshape(BS, 1, flat)


VMEM_LIMIT = 61 * 1024 * 1024


def solution(mesh):
    return jax.shard_map(
        on_device,
        mesh=mesh,
        in_specs=(
            P("row", "col", None),
            P("row", "col", None),
            P(None, "row", "col", None),
            P(None, "col", "row", None),
            P(None, "col", "row", None),
            P(None, "col", None),
        ),
        out_specs=P("row", "col", None),
        check_vma=False,
    )
```
